256 devices in a mesh: gx: 4 (over x), gy: 4 (over y), gz: 16 (over z, core).
Axes of the slice: x: 4, y: 4, z: 8, core: 2. Of those that a mesh axis runs over, the one named last changes fastest.
Arguments:
- log_probs: float32 [65536, 1024], P(('gx', 'gy', 'gz')), may hold values from -2 to 0
- ref_log_probs: float32 [65536, 1024], P(('gx', 'gy', 'gz')), may hold values from -2 to 0
- rewards: float32 [65536, 128], P(('gx', 'gy', 'gz')), may hold values from -6 to 6
- destination: int32 [65536], P(('gx', 'gy', 'gz')), may hold values from 0 to 65535, as said below
- lengths: int32 [65536], P(('gx', 'gy', 'gz')), may hold values from 1 to 1024
- mixing: float32 [128], replicated, may hold values from -0.5 to 0.5
Outputs:
- token_loss: float32 [65536, 1024], P(('gx', 'gy', 'gz'))
- advantages: float32 [65536, 128], P(('gx', 'gy', 'gz'))
The draws below stay inside these ranges and needn't reach their ends.
Inputs may be any that keep to these rules, and one draw needn't show every extreme that they name: A permutation. Rows are numbered along gx+gy+gz, 256 a device. Moving each row first to the gx index of its destination device, then to its gy index, then to its gz index, every device holds exactly 256 rows after each move, and at the three moves one device sends at most 128, 128 and 32 rows to one index, bounds reached in every draw.
All inputs are finite; a program needn't handle non-finite values.
Results may differ from the reference program's by a relative error of at most 0.0003.
Values sent between devices are 32-bit elements; how exact they have to be, the bound alone decides.
A program may use at most 64 MiB of HBM per device.

```python
import jax
import jax.numpy as jnp
from jax import lax

COMP_DEV = 256
SEQ = 1024
SCORES = 128
GROUP = 16
COMPLETIONS = 65536
N_GX = 4
N_GY = 4
N_GZ = 16


def draw_destination(key, part):
    devices = N_GX * N_GY * N_GZ
    overall = COMP_DEV * devices
    holder = jnp.arange(overall, dtype=jnp.int32) // COMP_DEV
    layout = ((N_GX, N_GY * N_GZ), (N_GY, N_GZ), (N_GZ, 1))
    for hop_index in range(3):
        fanout, stride = layout[hop_index]
        hop_key = jax.random.fold_in(key, 11 + hop_index)
        first_key, second_key, third_key = jax.random.split(hop_key, 3)
        capacity = 2 * COMP_DEV // fanout
        line_count = devices // fanout
        line_keys = jax.random.split(first_key, line_count)
        choosing = jax.vmap(lambda line_key: jax.random.permutation(line_key, fanout))(line_keys)
        counts = jnp.where(choosing < fanout // 2, capacity, 0).astype(jnp.int32)
        if fanout >= 4:
            shifted = jax.random.randint(second_key, (line_count, 1), 0, capacity, dtype=jnp.int32)
            counts = counts - jnp.where(choosing == 0, shifted, 0) + jnp.where(choosing == fanout // 2, shifted, 0)
        shuffle = jax.random.permutation(third_key, overall).astype(jnp.int32)
        ordering = jnp.argsort(holder * overall + shuffle, stable=True)
        ranking = jnp.zeros((overall,), jnp.int32).at[ordering].set(jnp.arange(overall, dtype=jnp.int32)) - holder * COMP_DEV
        coordinate = holder // stride % fanout
        line = holder // (stride * fanout) * stride + holder % stride
        bounds = jnp.cumsum(counts, axis=1)[line]
        offset = jnp.sum((ranking[:, None] >= bounds).astype(jnp.int32), axis=1)
        target = (coordinate + offset) % fanout
        holder = holder + (target - coordinate) * stride
    final_key = jax.random.fold_in(key, 17)
    shuffle = jax.random.permutation(final_key, overall).astype(jnp.int32)
    ordering = jnp.argsort(holder * overall + shuffle, stable=True)
    ranking = jnp.zeros((overall,), jnp.int32).at[ordering].set(jnp.arange(overall, dtype=jnp.int32)) - holder * COMP_DEV
    return holder * COMP_DEV + ranking


def plant(result, rng, low, largest):
    dims = result.shape
    place = [jax.random.randint(jax.random.fold_in(rng, axis), (), 0, dims[axis]) for axis in range(len(dims))]
    result = result.at[tuple(place)].set(low)
    longest = dims.index(max(dims))
    place[longest] = (place[longest] + 1) % dims[longest]
    return result.at[tuple(place)].set(largest)


def block_levels(stream_key, extent, pieces, low, largest):
    factor_of = 1.0
    for dim, blocks in pieces:
        steps = jax.random.uniform(jax.random.fold_in(jax.random.fold_in(stream_key, 6), dim), (blocks,), jnp.float32, low / len(pieces), largest / len(pieces))
        factor_of = factor_of * jnp.repeat(jnp.exp(steps), extent[dim] // blocks).reshape((-1,) + (1,) * (len(extent) - 1 - dim))
    return factor_of


def scatter_about(own_key, extent, scale, bound, shards=(), kind=jnp.bfloat16):
    loudness = block_levels(own_key, extent, shards, -0.22, 0.18) if shards else 1.0
    values = jax.random.normal(own_key, extent, jnp.float32) * scale * loudness
    return jnp.minimum(jnp.maximum(values, -bound), bound).astype(kind)


def setup_inputs(seed: int = 0) -> dict:
    streams_of = jax.random.split(jax.random.key(seed), 7)
    log_probs = jnp.clip(-2.0 + 2.0 * jax.random.uniform(streams_of[0], (COMPLETIONS, SEQ), jnp.float32) ** block_levels(streams_of[0], (COMPLETIONS, SEQ), ((0, 256),), -0.2, 0.2), -2.0, 0.0)
    ref_log_probs = jnp.clip(-2.0 + 2.0 * jax.random.uniform(streams_of[1], (COMPLETIONS, SEQ), jnp.float32) ** block_levels(streams_of[1], (COMPLETIONS, SEQ), ((0, 256),), -0.2, 0.2), -2.0, 0.0)
    rewards = scatter_about(streams_of[2], (COMPLETIONS, SCORES), 1.0, 6.0, ((0, 256),), jnp.float32)
    destination = draw_destination(jax.random.fold_in(streams_of[6], 71), 0)
    lengths = plant(jax.random.randint(streams_of[4], (COMPLETIONS,), 1, SEQ + 1), jax.random.fold_in(streams_of[4], 1), 1, SEQ).astype(jnp.int32)
    mixing = scatter_about(streams_of[5], (SCORES,), SCORES ** -0.5, 0.5, (), jnp.float32)
    return {"log_probs": log_probs, "ref_log_probs": ref_log_probs, "rewards": rewards, "destination": destination, "lengths": lengths, "mixing": mixing}


beta = 0.2

def reference(log_probs, ref_log_probs, rewards, destination, lengths, mixing):
    overall = destination.shape[0]
    source = jnp.zeros((overall,), jnp.int32).at[destination].set(jnp.arange(overall, dtype=jnp.int32))
    reaches = lengths[source]
    policy = log_probs[source]
    older = ref_log_probs[source]
    judged = rewards[source]
    grouped = judged.reshape(overall // GROUP, GROUP, judged.shape[1])
    centre = lax.optimization_barrier(jnp.mean(grouped, axis=1, keepdims=True))
    deviation = grouped - centre
    spread = lax.optimization_barrier(jnp.mean(deviation * deviation, axis=1, keepdims=True))
    advantages = (deviation / jnp.sqrt(spread + 1.0)).reshape(overall, judged.shape[1])
    weight = jnp.dot(advantages, mixing, precision=lax.Precision.HIGHEST)
    log_gap = older - policy
    penalty = jnp.exp(log_gap) - log_gap - 1.0
    inside = jnp.arange(policy.shape[1], dtype=jnp.int32)[None, :] < reaches[:, None]
    token_loss = jnp.where(inside, beta * penalty - weight[:, None] * policy, jnp.float32(0.0))
    return (token_loss, advantages)
```

```python
import functools

import jax
import jax.numpy as jnp
from jax import lax
from jax.experimental import pallas as pl
from jax.experimental.pallas import tpu as pltpu
from jax.sharding import PartitionSpec as P

GROUP = 16
BETA = 0.2
LANES = 128
HEAD = 8
MESH = pl.DeviceIdType.MESH
F32 = jnp.float32
BF16 = jnp.bfloat16


def log2(n):
    return n.bit_length() - 1


def iota(shape, dim):
    return lax.broadcasted_iota(jnp.int32, shape, dim)


def dot(a, b):
    return jnp.dot(a, b, preferred_element_type=F32)


def pick(onehot, x, terms):
    total, rest = None, x
    for t in range(terms):
        part = rest.astype(BF16)
        if t < terms - 1:
            rest = rest - part.astype(F32)
        got = dot(onehot, part)
        total = got if total is None else total + got
    return total


def to_column(row):
    n = row.shape[1]
    parts = []
    for t in range(n // LANES):
        tile = row[:, t * LANES : (t + 1) * LANES]
        eye = iota((LANES, LANES), 0) == iota((LANES, LANES), 1)
        parts.append(
            jnp.sum(jnp.where(eye, jnp.broadcast_to(tile, (LANES, LANES)), 0.0), axis=1, keepdims=True)
        )
    return jnp.concatenate(parts, axis=0)


def kernel(
    sizes, chunks, dest_ref, len_ref, mix_ref, lp_ref, rp_ref, rw_ref, tok_ref, adv_ref,
    upper, hot1, hot2, hot3, hot4, lens, wcol,
    rxs, rxr, rys, ryr, rzs, rzr, ws, wr,
    xs, xr, ys, yr, zg, zs, zr,
    rsend, rrecv, xsend, xrecv, ysend, yrecv, zsend, zrecv,
):
    nx, ny, nz = sizes
    rows = lp_ref.shape[0]
    slots = 2 * rows
    cx, cy, cz = slots // nx, slots // ny, slots // nz
    per_tile = LANES // cz
    mx, my, mz = lax.axis_index("gx"), lax.axis_index("gy"), lax.axis_index("gz")
    ring = {"gx": (mx, nx), "gy": (my, ny), "gz": (mz, nz)}

    def peer(axis, step):
        me, n = ring[axis]
        return {axis: lax.rem(me + (step + n), n)}

    barrier = pltpu.get_barrier_semaphore()
    for axis in ("gx", "gy", "gz"):
        for k in range(1, ring[axis][1]):
            pl.semaphore_signal(barrier, inc=1, device_id=peer(axis, k), device_id_type=MESH)

    def send(axis, k, src, dst, ssem, rsem):
        pltpu.make_async_remote_copy(
            src_ref=src, dst_ref=dst, send_sem=ssem, recv_sem=rsem,
            device_id=peer(axis, k), device_id_type=MESH,
        ).start()

    def drain(ref, sem):
        pltpu.make_async_copy(ref, ref, sem).wait()

    upper[...] = jnp.where(iota((slots, slots), 0) < iota((slots, slots), 1), 1.0, 0.0).astype(BF16)

    def slots_of(digit, valid, me, fanout, capacity):
        n = digit.shape[1]
        step = lax.rem(digit - me + fanout, fanout)
        groups = max(fanout, 8)
        member = jnp.where((iota((groups, n), 0) == step) & valid, 1.0, 0.0)
        before = dot(member.astype(BF16), upper[0:n, 0:n])
        rank = jnp.sum(member * before, axis=0, keepdims=True).astype(jnp.int32)
        return jnp.where(valid, step * capacity + rank, -1)

    def one_hot(slot, count):
        n = slot.shape[1]
        return jnp.where(iota((count, n), 0) == slot, 1.0, 0.0).astype(BF16)

    def carry(head, hot):
        return lax.dot_general(
            head.astype(BF16), hot, (((1,), (1,)), ((), ())), preferred_element_type=F32
        )

    dest = jnp.concatenate([dest_ref[t : t + 1, :] for t in range(rows // LANES)], axis=1)
    tx = dest >> log2(rows * ny * nz)
    ty = (dest >> log2(rows * nz)) & (ny - 1)
    tz = (dest >> log2(rows)) & (nz - 1)
    local = dest & (rows - 1)
    field = iota((HEAD, rows), 0)
    head = jnp.where(
        field == 0, ty, jnp.where(field == 1, tz, jnp.where(field == 2, local, jnp.where(field == 3, 1, 0)))
    ).astype(F32)
    hot1[...] = one_hot(slots_of(tx, dest >= 0, mx, nx, cx), slots)
    head = carry(head, hot1[...])
    got = pick(hot1[...], rw_ref[...], 3)
    for k in range(nx):
        to = rxr if k == 0 else rxs
        to[k, 0:HEAD, :] = head[:, k * cx : (k + 1) * cx]
        to[k, HEAD:, :] = got[k * cx : (k + 1) * cx, :]
    pl.semaphore_wait(barrier, (nx - 1) + (ny - 1) + (nz - 1))
    for k in range(1, nx):
        send("gx", k, rxs.at[k], rxr.at[k], rsend.at[0], rrecv.at[0])

    len_row = jnp.concatenate([len_ref[t : t + 1, :] for t in range(rows // LANES)], axis=1)
    lens[...] = jnp.broadcast_to(to_column(len_row.astype(F32)), (rows, LANES)).astype(jnp.int32)

    @pl.loop(0, chunks)
    def _(c):
        columns = pl.ds(pl.multiple_of(c * LANES, LANES), LANES)
        inside = (iota((rows, LANES), 1) + c * LANES) < lens[...]
        policy = lp_ref[:, columns]
        gap = rp_ref[:, columns] - policy
        penalty = jnp.exp(gap) - gap - 1.0
        both = jnp.concatenate(
            [jnp.where(inside, policy, 0.0), jnp.where(inside, BETA * penalty, 0.0)], axis=1
        )
        got = pick(hot1[...], both, 2)
        xr[c, 0:cx, :] = got[0:cx, :]
        xs[c] = got
        for k in range(1, nx):
            at = pl.ds(k * cx, cx)
            send("gx", k, xs.at[c, at], xr.at[c, at], xsend.at[c], xrecv.at[c])

    drain(rxr.at[pl.ds(1, nx - 1)], rrecv.at[0])
    head = jnp.concatenate([rxr[k, 0:HEAD, :] for k in range(nx)], axis=1)
    held = head.astype(jnp.int32)
    hot2[...] = one_hot(slots_of(held[0:1, :], held[3:4, :] > 0, my, ny, cy), slots)
    head = carry(head, hot2[...])
    got = pick(hot2[...], rxr[:, HEAD:, :].reshape(slots, LANES), 3)
    for k in range(ny):
        to = ryr if k == 0 else rys
        to[k, 0:HEAD, :] = head[:, k * cy : (k + 1) * cy]
        to[k, HEAD:, :] = got[k * cy : (k + 1) * cy, :]
    for k in range(1, ny):
        send("gy", k, rys.at[k], ryr.at[k], rsend.at[1], rrecv.at[1])

    def to_y(c):
        drain(xr.at[c, pl.ds(cx, slots - cx)], xrecv.at[c])
        got = pick(hot2[...], xr[c], 2)
        yr[c, 0:cy, :] = got[0:cy, :]
        ys[c] = got
        for k in range(1, ny):
            at = pl.ds(k * cy, cy)
            send("gy", k, ys.at[c, at], yr.at[c, at], ysend.at[c], yrecv.at[c])

    drain(ryr.at[pl.ds(1, ny - 1)], rrecv.at[1])
    head = jnp.concatenate([ryr[k, 0:HEAD, :] for k in range(ny)], axis=1)
    held = head.astype(jnp.int32)
    hot3[...] = one_hot(slots_of(held[1:2, :], held[3:4, :] > 0, mz, nz, cz), slots)
    head = carry(head, hot3[...])
    got = pick(hot3[...], ryr[:, HEAD:, :].reshape(slots, LANES), 3)
    for k in range(nz):
        to = rzr if k == 0 else rzs
        tile = k // per_tile * LANES
        to[k, 0:HEAD, :] = head[:, tile : tile + LANES]
        to[k, HEAD:, :] = got[k * cz : (k + 1) * cz, :]
    for k in range(1, nz):
        send("gz", k, rzs.at[k], rzr.at[k], rsend.at[2], rrecv.at[2])

    def along_slots(tiles):
        spot = iota((HEAD, LANES), 1) // cz
        parts = []
        for t in range(nz // per_tile):
            part = tiles(t * per_tile)
            for j in range(1, per_tile):
                part = jnp.where(spot == j, tiles(t * per_tile + j), part)
            parts.append(part)
        return jnp.concatenate(parts, axis=1)

    to_y(0)
    to_y(1)

    drain(rzr.at[pl.ds(1, nz - 1)], rrecv.at[2])
    held = along_slots(lambda k: rzr[k, 0:HEAD, :]).astype(jnp.int32)
    place = jnp.where(held[3:4, :] > 0, held[2:3, :], -1)
    chosen = iota((rows, slots), 0) == place
    hot4[...] = jnp.where(chosen, 1.0, 0.0).astype(BF16)
    judged = pick(hot4[...], rzr[:, HEAD:, :].reshape(slots, LANES), 3)
    grouped = judged.reshape(rows // GROUP, GROUP, LANES)
    centre = jnp.mean(grouped, axis=1, keepdims=True)
    deviation = grouped - centre
    spread = jnp.mean(deviation * deviation, axis=1, keepdims=True)
    advantages = (deviation / jnp.sqrt(spread + 1.0)).reshape(rows, LANES)
    adv_ref[...] = advantages
    weight = jnp.sum(advantages * mix_ref[...], axis=1, keepdims=True)
    row = jnp.sum(jnp.where(chosen, weight, 0.0), axis=0, keepdims=True)
    for t in range(nz // per_tile):
        ws[t] = jnp.broadcast_to(row[:, t * LANES : (t + 1) * LANES], (HEAD, LANES))
    wr[0] = jnp.broadcast_to(row[:, 0:LANES], (HEAD, LANES))
    for k in range(1, nz):
        send("gz", -k, ws.at[k // per_tile], wr.at[k], rsend.at[3], rrecv.at[3])

    def gather_z(c):
        drain(yr.at[c, pl.ds(cy, slots - cy)], yrecv.at[c])
        zg[c] = pick(hot3[...], yr[c], 2)

    def send_z(c):
        loss = zg[c, :, LANES:] - wcol[...] * zg[c, :, 0:LANES]
        zr[c, 0:cz, :] = loss[0:cz, :]
        zs[c] = loss
        for k in range(1, nz):
            at = pl.ds(k * cz, cz)
            send("gz", k, zs.at[c, at], zr.at[c, at], zsend.at[c], zrecv.at[c])

    gather_z(0)
    drain(wr.at[pl.ds(1, nz - 1)], rrecv.at[3])
    wcol[...] = jnp.broadcast_to(to_column(along_slots(lambda k: wr[k])[0:1, :]), (slots, LANES))
    send_z(0)

    @pl.loop(2, chunks)
    def _(c):
        to_y(c)
        gather_z(c - 1)
        send_z(c - 1)

    gather_z(chunks - 1)
    send_z(chunks - 1)

    @pl.loop(0, chunks)
    def _(c):
        drain(zr.at[c, pl.ds(cz, slots - cz)], zrecv.at[c])
        columns = pl.ds(pl.multiple_of(c * LANES, LANES), LANES)
        tok_ref[:, columns] = pick(hot4[...], zr[c], 2)

    drain(rxs.at[pl.ds(1, nx - 1)], rsend.at[0])
    drain(rys.at[pl.ds(1, ny - 1)], rsend.at[1])
    drain(rzs.at[pl.ds(1, nz - 1)], rsend.at[2])
    drain(wr.at[pl.ds(1, nz - 1)], rsend.at[3])

    @pl.loop(0, chunks)
    def _(c):
        drain(xs.at[c, pl.ds(cx, slots - cx)], xsend.at[c])
        drain(ys.at[c, pl.ds(cy, slots - cy)], ysend.at[c])
        drain(zs.at[c, pl.ds(cz, slots - cz)], zsend.at[c])


def on_device(sizes, log_probs, ref_log_probs, rewards, destination, lengths, mixing):
    rows, width = log_probs.shape
    slots = 2 * rows
    chunks = width // LANES
    nx, ny, nz = sizes
    vmem = pl.BlockSpec(memory_space=pltpu.VMEM)
    wide = pltpu.VMEM((chunks, slots, 2 * LANES), F32)
    thin = pltpu.VMEM((chunks, slots, LANES), F32)
    sem = pltpu.SemaphoreType.DMA

    def reward_buffer(n):
        return pltpu.VMEM((n, HEAD + slots // n, LANES), F32)

    return pl.pallas_call(
        functools.partial(kernel, sizes, chunks),
        out_shape=(
            jax.ShapeDtypeStruct((rows, width), F32),
            jax.ShapeDtypeStruct((rows, LANES), F32),
        ),
        in_specs=[vmem] * 6,
        out_specs=(vmem, vmem),
        scratch_shapes=[
            pltpu.VMEM((slots, slots), BF16),
            pltpu.VMEM((slots, rows), BF16),
            pltpu.VMEM((slots, slots), BF16),
            pltpu.VMEM((slots, slots), BF16),
            pltpu.VMEM((rows, slots), BF16),
            pltpu.VMEM((rows, LANES), jnp.int32),
            pltpu.VMEM((slots, LANES), F32),
            reward_buffer(nx), reward_buffer(nx),
            reward_buffer(ny), reward_buffer(ny),
            reward_buffer(nz), reward_buffer(nz),
            pltpu.VMEM((slots // LANES, HEAD, LANES), F32),
            pltpu.VMEM((nz, HEAD, LANES), F32),
            wide, wide, wide, wide, wide, thin, thin,
            sem((4,)), sem((4,)),
            sem((chunks,)), sem((chunks,)), sem((chunks,)), sem((chunks,)), sem((chunks,)), sem((chunks,)),
        ],
        compiler_params=pltpu.CompilerParams(
            collective_id=0, has_side_effects=True, vmem_limit_bytes=60 << 20
        ),
        name="regroup",
    )(
        destination.reshape(rows // LANES, LANES),
        lengths.reshape(rows // LANES, LANES),
        mixing.reshape(1, LANES),
        log_probs,
        ref_log_probs,
        rewards,
    )


def solution(mesh):
    sizes = tuple(mesh.shape[a] for a in ("gx", "gy", "gz"))
    rows = P(("gx", "gy", "gz"), None)
    flat = P(("gx", "gy", "gz"))
    return jax.shard_map(
        functools.partial(on_device, sizes),
        mesh=mesh,
        in_specs=(rows, rows, rows, flat, flat, P()),
        out_specs=(rows, rows),
        check_vma=False,
    )
```

```python
import functools

import jax
import jax.numpy as jnp
from jax import lax
from jax.experimental import pallas as pl
from jax.experimental.pallas import tpu as pltpu
from jax.sharding import PartitionSpec as P

GROUP = 16
BETA = 0.2
LANES = 128
HALF = LANES // 2
HEAD = 8
MESH = pl.DeviceIdType.MESH
F32 = jnp.float32
BF16 = jnp.bfloat16


def log2(n):
    return n.bit_length() - 1


def iota(shape, dim):
    return lax.broadcasted_iota(jnp.int32, shape, dim)


def dot(a, b):
    return jnp.dot(a, b, preferred_element_type=F32)


def pick(onehot, x, terms):
    total, rest = None, x
    for t in range(terms):
        part = rest.astype(BF16)
        if t < terms - 1:
            rest = rest - part.astype(F32)
        got = dot(onehot, part)
        total = got if total is None else total + got
    return total


def low():
    return iota((1, LANES), 1) < HALF


def swap(x):
    return pltpu.roll(x, HALF, 1)


def to_column(row):
    n = row.shape[1]
    parts = []
    for t in range(n // LANES):
        tile = row[:, t * LANES : (t + 1) * LANES]
        eye = iota((LANES, LANES), 0) == iota((LANES, LANES), 1)
        parts.append(
            jnp.sum(jnp.where(eye, jnp.broadcast_to(tile, (LANES, LANES)), 0.0), axis=1, keepdims=True)
        )
    return jnp.concatenate(parts, axis=0)


def kernel(
    sizes, chunks, dest_hbm, len_hbm, mix_hbm, lp_hbm, rp_hbm, rw_hbm, tok_ref, adv_ref,
    dest_ref, len_ref, mix_ref, lp_ref, rp_ref, rw_ref,
    upper, hot1, hot2, hot3, hot4, lens, wcol, wrow,
    hxs, hxr, hys, hyr, hzs, hzr, ws, wr,
    rxs, rxr, rys, ryr, rzs, rzr,
    xs, xr, ys, yr, zg, zs, zr,
    loads, hsend, hrecv, rsend, rrecv, xsend, xrecv, ysend, yrecv, zsend, zrecv,
):
    nx, ny, nz = sizes
    rows = lp_ref.shape[0]
    slots = 2 * rows
    cx, cy, cz = slots // nx, slots // ny, slots // nz
    per_tile = LANES // cz
    tiles = slots // LANES
    mx, my, mz = lax.axis_index("gx"), lax.axis_index("gy"), lax.axis_index("gz")
    ring = {"gx": (mx, nx), "gy": (my, ny), "gz": (mz, nz)}

    def far_first(n):
        return sorted(range(1, n), key=lambda k: -min(k, n - k))

    def peer(axis, step):
        me, n = ring[axis]
        return {axis: lax.rem(me + (step + n), n)}

    fetches = [
        pltpu.make_async_copy(a, b, loads.at[i])
        for i, (a, b) in enumerate(
            (
                (dest_hbm, dest_ref), (rw_hbm, rw_ref), (len_hbm, len_ref),
                (lp_hbm, lp_ref), (rp_hbm, rp_ref), (mix_hbm, mix_ref),
            )
        )
    ]
    for fetch in fetches:
        fetch.start()

    barrier = pltpu.get_barrier_semaphore()
    for axis in ("gz", "gx", "gy"):
        for k in range(1, ring[axis][1]):
            pl.semaphore_signal(barrier, inc=1, device_id=peer(axis, k), device_id_type=MESH)

    def send(axis, k, src, dst, ssem, rsem):
        pltpu.make_async_remote_copy(
            src_ref=src, dst_ref=dst, send_sem=ssem, recv_sem=rsem,
            device_id=peer(axis, k), device_id_type=MESH,
        ).start()

    def drain(ref, sem):
        pltpu.make_async_copy(ref, ref, sem).wait()

    upper[...] = jnp.where(iota((slots, slots), 0) < iota((slots, slots), 1), 1.0, 0.0).astype(BF16)

    def slots_of(digit, valid, me, fanout, capacity):
        n = digit.shape[1]
        step = lax.rem(digit - me + fanout, fanout)
        groups = max(fanout, 8)
        member = jnp.where((iota((groups, n), 0) == step) & valid, 1.0, 0.0)
        before = dot(member.astype(BF16), upper[0:n, 0:n])
        rank = jnp.sum(member * before, axis=0, keepdims=True).astype(jnp.int32)
        return jnp.where(valid, step * capacity + rank, -1)

    def one_hot(slot, count):
        n = slot.shape[1]
        return jnp.where(iota((count, n), 0) == slot, 1.0, 0.0).astype(BF16)

    def carry(head, hot):
        return lax.dot_general(
            head.astype(BF16), hot, (((1,), (1,)), ((), ())), preferred_element_type=F32
        )

    def spread_rewards(hot, x, n, own, out):
        got = pick(hot, x, 3)
        c = slots // n // 2
        first = got.reshape(n, 2, c, LANES)[:, 0]
        last = swap(got).reshape(n, 2, c, LANES)[:, 1]
        packed = jnp.where(low()[None], first, last)
        own[0] = packed[0]
        out[...] = packed

    def unpacked(ref):
        n, c = ref.shape[0], ref.shape[1]
        x = ref[...]
        y = swap(x.reshape(n * c, LANES)).reshape(n, c, LANES)
        return jnp.concatenate([x, y], axis=1).reshape(slots, LANES)

    def along_slots(tile):
        spot = iota((HEAD, LANES), 1) // cz
        parts = []
        for t in range(tiles):
            part = tile(t * per_tile)
            for j in range(1, per_tile):
                part = jnp.where(spot == j, tile(t * per_tile + j), part)
            parts.append(part)
        return jnp.concatenate(parts, axis=1)

    fetches[0].wait()
    dest = jnp.concatenate([dest_ref[t : t + 1, :] for t in range(rows // LANES)], axis=1)
    tx = dest >> log2(rows * ny * nz)
    ty = (dest >> log2(rows * nz)) & (ny - 1)
    tz = (dest >> log2(rows)) & (nz - 1)
    local = dest & (rows - 1)
    field = iota((HEAD, rows), 0)
    head = jnp.where(
        field == 0, ty, jnp.where(field == 1, tz, jnp.where(field == 2, local, jnp.where(field == 3, 1, 0)))
    ).astype(F32)
    hot1[...] = one_hot(slots_of(tx, dest >= 0, mx, nx, cx), slots)
    head = carry(head, hot1[...])
    hxr[0] = head[:, 0:cx]
    for k in range(1, nx):
        hxs[k] = head[:, k * cx : (k + 1) * cx]
    fetches[1].wait()
    spread_rewards(hot1[...], rw_ref[...], nx, rxr.at[0], rxs.at[0])
    def send_rewards(axis, hop, half, out, into):
        for k in far_first(ring[axis][1]):
            at = 2 * hop + half
            send(axis, k, out.at[half, k], into.at[half, k], rsend.at[at], rrecv.at[at])

    def drain_rewards(hop, half, ref, sem):
        drain(ref.at[half, pl.ds(1, ref.shape[1] - 1)], sem.at[2 * hop + half])

    pl.semaphore_wait(barrier, (nx - 1) + (ny - 1) + (nz - 1))
    send_rewards("gx", 0, 0, rxs, rxr)
    for k in far_first(nx):
        send("gx", k, hxs.at[k], hxr.at[k], hsend.at[0], hrecv.at[0])
    spread_rewards(hot1[...], swap(rw_ref[...]), nx, rxr.at[1], rxs.at[1])
    send_rewards("gx", 0, 1, rxs, rxr)
    fetches[2].wait()
    len_row = jnp.concatenate([len_ref[t : t + 1, :] for t in range(rows // LANES)], axis=1)
    lens[...] = jnp.broadcast_to(to_column(len_row.astype(F32)), (rows, LANES)).astype(jnp.int32)
    fetches[3].wait()
    fetches[4].wait()

    def to_x(c):
        columns = pl.ds(pl.multiple_of(c * LANES, LANES), LANES)
        inside = (iota((rows, LANES), 1) + c * LANES) < lens[...]
        policy = lp_ref[:, columns]
        gap = rp_ref[:, columns] - policy
        penalty = jnp.exp(gap) - gap - 1.0
        policy = jnp.where(inside, policy, 0.0)
        penalty = jnp.where(inside, BETA * penalty, 0.0)
        other = swap(policy)
        both = jnp.concatenate(
            [jnp.where(low(), penalty, other), jnp.where(low(), other, penalty)], axis=1
        )
        got = pick(hot1[...], both, 2)
        for h in range(2):
            part = got[:, h * LANES : (h + 1) * LANES]
            xr[2 * c + h, 0:cx, :] = part[0:cx, :]
            xs[2 * c + h] = part
            for k in far_first(nx):
                at = pl.ds(k * cx, cx)
                send(
                    "gx", k, xs.at[2 * c + h, at], xr.at[2 * c + h, at],
                    xsend.at[2 * c + h], xrecv.at[2 * c + h],
                )

    def to_y(c):
        drain(xr.at[c, pl.ds(cx, slots - cx)], xrecv.at[c])
        got = pick(hot2[...], xr[c], 2)
        yr[c, 0:cy, :] = got[0:cy, :]
        ys[c] = got
        for k in far_first(ny):
            at = pl.ds(k * cy, cy)
            send("gy", k, ys.at[c, at], yr.at[c, at], ysend.at[c], yrecv.at[c])

    def drain_y(c):
        drain(yr.at[c, pl.ds(cy, slots - cy)], yrecv.at[c])

    def gather_z(c):
        drain_y(2 * c)
        drain_y(2 * c + 1)
        return pick(hot3[...], jnp.concatenate([yr[2 * c], yr[2 * c + 1]], axis=1), 2)

    def loss(even, odd, weights):
        return jnp.where(low(), even, odd) - weights * swap(jnp.where(low(), odd, even))

    def send_z(c, rows_out):
        zr[c, 0:cz, :] = rows_out[0:cz, :]
        zs[c] = rows_out
        for k in far_first(nz):
            at = pl.ds(k * cz, cz)
            send("gz", k, zs.at[c, at], zr.at[c, at], zsend.at[c], zrecv.at[c])

    to_x(0)

    drain(hxr.at[pl.ds(1, nx - 1)], hrecv.at[0])
    head = jnp.concatenate([hxr[k] for k in range(nx)], axis=1)
    held = head.astype(jnp.int32)
    hot2[...] = one_hot(slots_of(held[0:1, :], held[3:4, :] > 0, my, ny, cy), slots)
    head = carry(head, hot2[...])
    hyr[0] = head[:, 0:cy]
    for k in range(1, ny):
        hys[k] = head[:, k * cy : (k + 1) * cy]
    for k in far_first(ny):
        send("gy", k, hys.at[k], hyr.at[k], hsend.at[1], hrecv.at[1])

    for half in range(2):
        drain_rewards(0, half, rxr, rrecv)
        spread_rewards(hot2[...], unpacked(rxr.at[half]), ny, ryr.at[half], rys.at[half])
        send_rewards("gy", 1, half, rys, ryr)

    to_x(1)

    drain(hyr.at[pl.ds(1, ny - 1)], hrecv.at[1])
    head = jnp.concatenate([hyr[k] for k in range(ny)], axis=1)
    held = head.astype(jnp.int32)
    hot3[...] = one_hot(slots_of(held[1:2, :], held[3:4, :] > 0, mz, nz, cz), slots)
    head = carry(head, hot3[...])
    hzr[0] = head[:, 0:LANES]
    for t in range(tiles):
        hzs[t] = head[:, t * LANES : (t + 1) * LANES]
    for k in far_first(nz):
        send("gz", k, hzs.at[k // per_tile], hzr.at[k], hsend.at[2], hrecv.at[2])

    def rewards_to_z(half):
        drain_rewards(1, half, ryr, rrecv)
        spread_rewards(hot3[...], unpacked(ryr.at[half]), nz, rzr.at[half], rzs.at[half])
        send_rewards("gz", 2, half, rzs, rzr)

    rewards_to_z(0)
    to_y(0)
    rewards_to_z(1)
    to_x(2)
    drain(hzr.at[pl.ds(1, nz - 1)], hrecv.at[2])
    held = along_slots(lambda k: hzr[k]).astype(jnp.int32)
    place = jnp.where(held[3:4, :] > 0, held[2:3, :], -1)
    hot4[...] = jnp.where(iota((rows, slots), 0) == place, 1.0, 0.0).astype(BF16)
    to_y(1)
    to_x(3)
    fetches[5].wait()

    drain_y(0)
    send_z(0, pick(hot3[...], yr[0], 2))
    to_y(2)
    to_x(4)
    to_y(3)
    drain_y(1)
    zg[...] = pick(hot3[...], yr[1], 2)

    drain_rewards(2, 0, rzr, rrecv)
    judged = pick(hot4[...], unpacked(rzr.at[0]), 3)
    drain_rewards(2, 1, rzr, rrecv)
    judged = jnp.where(low(), judged, swap(pick(hot4[...], unpacked(rzr.at[1]), 3)))
    grouped = judged.reshape(rows // GROUP, GROUP, LANES)
    centre = jnp.mean(grouped, axis=1, keepdims=True)
    deviation = grouped - centre
    spread = jnp.mean(deviation * deviation, axis=1, keepdims=True)
    advantages = (deviation / jnp.sqrt(spread + 1.0)).reshape(rows, LANES)
    weight = jnp.sum(advantages * mix_ref[...], axis=1, keepdims=True)
    row = jnp.sum(hot4[...].astype(F32) * weight, axis=0, keepdims=True)
    wr[0] = jnp.broadcast_to(row[:, 0:LANES], (HEAD, LANES))
    for t in range(tiles):
        ws[t] = jnp.broadcast_to(row[:, t * LANES : (t + 1) * LANES], (HEAD, LANES))
    for k in far_first(nz):
        send("gz", -k, ws.at[k // per_tile], wr.at[k], rsend.at[6], rrecv.at[6])
    send_z(chunks, zg[...])
    adv_ref[...] = advantages
    wrow[...] = jnp.broadcast_to(weight, (rows, LANES))

    to_y(4)
    to_x(5)
    to_y(5)
    second = gather_z(1)
    to_y(6)
    drain(wr.at[pl.ds(1, nz - 1)], rrecv.at[6])
    wcol[...] = jnp.broadcast_to(to_column(along_slots(lambda k: wr[k])[0:1, :]), (slots, LANES))
    send_z(1, loss(second[:, 0:LANES], second[:, LANES:], wcol[...]))
    to_x(6)
    to_y(7)
    to_x(7)

    def loss_to_z(c):
        got = gather_z(c)
        send_z(c, loss(got[:, 0:LANES], got[:, LANES:], wcol[...]))

    @pl.loop(2, chunks - 2)
    def _(c):
        loss_to_z(c)
        to_y(2 * c + 4)
        to_y(2 * c + 5)

    @pl.loop(chunks - 2, chunks)
    def _(c):
        loss_to_z(c)

    for i, (h, r, n) in enumerate(((hxr, rxr, nx), (hyr, ryr, ny), (hzr, rzr, nz))):
        drain(h.at[pl.ds(1, n - 1)], hsend.at[i])
        drain_rewards(i, 0, r, rsend)
        drain_rewards(i, 1, r, rsend)
    drain(wr.at[pl.ds(1, nz - 1)], rsend.at[6])

    @pl.loop(0, 2 * chunks)
    def _(c):
        drain(xs.at[c, pl.ds(cx, slots - cx)], xsend.at[c])
        drain(ys.at[c, pl.ds(cy, slots - cy)], ysend.at[c])

    def arrived(c):
        drain(zr.at[c, pl.ds(cz, slots - cz)], zrecv.at[c])
        return pick(hot4[...], zr[c], 2)

    even = arrived(0)
    tok_ref[:, 0:LANES] = loss(even, arrived(chunks), wrow[...])

    @pl.loop(1, chunks)
    def _(c):
        columns = pl.ds(pl.multiple_of(c * LANES, LANES), LANES)
        tok_ref[:, columns] = arrived(c)

    @pl.loop(0, chunks + 1)
    def _(c):
        drain(zs.at[c, pl.ds(cz, slots - cz)], zsend.at[c])


def on_device(sizes, log_probs, ref_log_probs, rewards, destination, lengths, mixing):
    rows, width = log_probs.shape
    slots = 2 * rows
    chunks = width // LANES
    nx, ny, nz = sizes
    wide = pltpu.VMEM((2 * chunks, slots, LANES), F32)
    thin = pltpu.VMEM((chunks + 1, slots, LANES), F32)
    sem = pltpu.SemaphoreType.DMA

    def head_buffer(n):
        return pltpu.VMEM((n, HEAD, LANES), F32)

    def reward_buffer(n):
        return pltpu.VMEM((2, n, slots // n // 2, LANES), F32)

    return pl.pallas_call(
        functools.partial(kernel, sizes, chunks),
        out_shape=(pltpu.VMEM((rows, width), F32), pltpu.VMEM((rows, LANES), F32)),
        in_specs=[pl.BlockSpec(memory_space=pl.ANY)] * 6,
        out_specs=(pl.BlockSpec(memory_space=pltpu.VMEM),) * 2,
        scratch_shapes=[
            pltpu.VMEM((rows // LANES, LANES), jnp.int32),
            pltpu.VMEM((rows // LANES, LANES), jnp.int32),
            pltpu.VMEM((1, LANES), F32),
            pltpu.VMEM((rows, width), F32),
            pltpu.VMEM((rows, width), F32),
            pltpu.VMEM((rows, LANES), F32),
            pltpu.VMEM((slots, slots), BF16),
            pltpu.VMEM((slots, rows), BF16),
            pltpu.VMEM((slots, slots), BF16),
            pltpu.VMEM((slots, slots), BF16),
            pltpu.VMEM((rows, slots), BF16),
            pltpu.VMEM((rows, LANES), jnp.int32),
            pltpu.VMEM((slots, LANES), F32),
            pltpu.VMEM((rows, LANES), F32),
            head_buffer(nx), head_buffer(nx),
            head_buffer(ny), head_buffer(ny),
            head_buffer(slots // LANES), head_buffer(nz),
            head_buffer(slots // LANES), head_buffer(nz),
            reward_buffer(nx), reward_buffer(nx),
            reward_buffer(ny), reward_buffer(ny),
            reward_buffer(nz), reward_buffer(nz),
            wide, wide, wide, wide, pltpu.VMEM((slots, LANES), F32), thin, thin,
            sem((6,)), sem((3,)), sem((3,)), sem((7,)), sem((7,)),
            sem((2 * chunks,)), sem((2 * chunks,)), sem((2 * chunks,)), sem((2 * chunks,)), sem((chunks + 1,)), sem((chunks + 1,)),
        ],
        compiler_params=pltpu.CompilerParams(
            collective_id=0, has_side_effects=True, vmem_limit_bytes=60 << 20
        ),
        name="regroup",
    )(
        destination.reshape(rows // LANES, LANES),
        lengths.reshape(rows // LANES, LANES),
        mixing.reshape(1, LANES),
        log_probs,
        ref_log_probs,
        rewards,
    )


def solution(mesh):
    sizes = tuple(mesh.shape[a] for a in ("gx", "gy", "gz"))
    rows = P(("gx", "gy", "gz"), None)
    flat = P(("gx", "gy", "gz"))
    return jax.shard_map(
        functools.partial(on_device, sizes),
        mesh=mesh,
        in_specs=(rows, rows, rows, flat, flat, P()),
        out_specs=(rows, rows),
        check_vma=False,
    )
```

```python
import functools

import jax
import jax.numpy as jnp
from jax import lax
from jax.experimental import pallas as pl
from jax.experimental.pallas import tpu as pltpu
from jax.sharding import PartitionSpec as P

GROUP = 16
BETA = 0.2
LANES = 128
HALF = LANES // 2
HEAD = 8
MESH = pl.DeviceIdType.MESH
F32 = jnp.float32
BF16 = jnp.bfloat16


def log2(n):
    return n.bit_length() - 1


def iota(shape, dim):
    return lax.broadcasted_iota(jnp.int32, shape, dim)


def dot(a, b):
    return jnp.dot(a, b, preferred_element_type=F32)


def pick(onehot, x):
    n = x.shape[1]
    first = x.astype(BF16)
    second = (x - first.astype(F32)).astype(BF16)
    got = dot(onehot, jnp.concatenate([first, second], axis=1))
    return got[:, 0:n] + got[:, n:]


def low():
    return iota((1, LANES), 1) < HALF


def swap(x):
    return pltpu.roll(x, HALF, 1)


def pick_half(onehot, x):
    first = x.astype(BF16).astype(F32)
    rest = x - first
    second = rest.astype(BF16).astype(F32)
    third = (rest - second).astype(BF16)
    both = jnp.where(low(), first, swap(second)).astype(BF16)
    got = dot(onehot, jnp.concatenate([both, third], axis=1))
    return (got[:, 0:LANES] + swap(got[:, 0:LANES])) + got[:, LANES:]


def to_column(row):
    n = row.shape[1]
    parts = []
    for t in range(n // LANES):
        tile = row[:, t * LANES : (t + 1) * LANES]
        eye = iota((LANES, LANES), 0) == iota((LANES, LANES), 1)
        parts.append(
            jnp.sum(jnp.where(eye, jnp.broadcast_to(tile, (LANES, LANES)), 0.0), axis=1, keepdims=True)
        )
    return jnp.concatenate(parts, axis=0)


def kernel(
    sizes, chunks, dest_hbm, len_hbm, mix_hbm, lp_hbm, rp_hbm, rw_hbm, tok_ref, adv_ref,
    dest_ref, len_ref, mix_ref, lp_ref, rp_ref, rw_ref,
    upper, hot1, hot2, hot3, hot4, lens, wcol, wrow,
    hxs, hxr, hys, hyr, hzs, hzr, ws, wr,
    rxs, rxr, rys, ryr, rzs, rzr,
    xs, xr, ys, yr, zs, zr,
    loads, hsend, hrecv, rsend, rrecv, xsend, xrecv, ysend, yrecv, zsend, zrecv,
):
    nx, ny, nz = sizes
    rows = lp_ref.shape[0]
    slots = 2 * rows
    cx, cy, cz = slots // nx, slots // ny, slots // nz
    per_tile = LANES // cz
    tiles = slots // LANES
    mx, my, mz = lax.axis_index("gx"), lax.axis_index("gy"), lax.axis_index("gz")
    ring = {"gx": (mx, nx), "gy": (my, ny), "gz": (mz, nz)}

    def far_first(n):
        return sorted(range(1, n), key=lambda k: -min(k, n - k))

    def peer(axis, step):
        me, n = ring[axis]
        return {axis: lax.rem(me + (step + n), n)}

    fetches = [
        pltpu.make_async_copy(a, b, loads.at[i])
        for i, (a, b) in enumerate(
            (
                (dest_hbm, dest_ref), (rw_hbm, rw_ref), (len_hbm, len_ref),
                (lp_hbm, lp_ref), (rp_hbm, rp_ref), (mix_hbm, mix_ref),
            )
        )
    ]
    for fetch in fetches:
        fetch.start()

    barrier = pltpu.get_barrier_semaphore()
    for axis in ("gz", "gx", "gy"):
        for k in range(1, ring[axis][1]):
            pl.semaphore_signal(barrier, inc=1, device_id=peer(axis, k), device_id_type=MESH)

    def send(axis, k, src, dst, ssem, rsem):
        pltpu.make_async_remote_copy(
            src_ref=src, dst_ref=dst, send_sem=ssem, recv_sem=rsem,
            device_id=peer(axis, k), device_id_type=MESH,
        ).start()

    def drain(ref, sem):
        pltpu.make_async_copy(ref, ref, sem).wait()

    upper[...] = jnp.where(iota((slots, slots), 0) < iota((slots, slots), 1), 1.0, 0.0).astype(BF16)

    def slots_of(digit, valid, me, fanout, capacity):
        n = digit.shape[1]
        step = lax.rem(digit - me + fanout, fanout)
        groups = max(fanout, 8)
        member = jnp.where((iota((groups, n), 0) == step) & valid, 1.0, 0.0)
        before = dot(member.astype(BF16), upper[0:n, 0:n])
        rank = jnp.sum(member * before, axis=0, keepdims=True).astype(jnp.int32)
        return jnp.where(valid, step * capacity + rank, -1)

    def one_hot(slot, count):
        n = slot.shape[1]
        return jnp.where(iota((count, n), 0) == slot, 1.0, 0.0).astype(BF16)

    def carry(head, hot):
        place = head - 1
        field = iota((HEAD, head.shape[1]), 0)
        parts = jnp.where(
            field == 0, place >> 8, jnp.where(field == 1, place & 255, jnp.where(field == 2, 1, 0))
        )
        parts = jnp.where(head > 0, parts, 0).astype(F32).astype(BF16)
        got = lax.dot_general(parts, hot, (((1,), (1,)), ((), ())), preferred_element_type=F32)
        return got[0:1, :] * 256.0 + got[1:2, :] + got[2:3, :]

    def spread_rewards(hot, x, n, own, out):
        got = pick_half(hot, x)
        c = slots // n // 2
        first = got.reshape(n, 2, c, LANES)[:, 0]
        last = swap(got).reshape(n, 2, c, LANES)[:, 1]
        packed = jnp.where(low()[None], first, last)
        own[0] = packed[0]
        out[...] = packed

    def unpacked(ref):
        n, c = ref.shape[0], ref.shape[1]
        x = ref[...]
        y = swap(x.reshape(n * c, LANES)).reshape(n, c, LANES)
        return jnp.concatenate([x, y], axis=1).reshape(slots, LANES)

    def along_slots(tile):
        spot = iota((1, LANES), 1) // cz
        parts = []
        for t in range(tiles):
            part = tile(t * per_tile)
            for j in range(1, per_tile):
                part = jnp.where(spot == j, tile(t * per_tile + j), part)
            parts.append(part)
        return jnp.concatenate(parts, axis=1)

    fetches[0].wait()
    dest = jnp.concatenate([dest_ref[t : t + 1, :] for t in range(rows // LANES)], axis=1)
    tx = dest >> log2(rows * ny * nz)
    hot1[...] = one_hot(slots_of(tx, dest >= 0, mx, nx, cx), slots)
    head = carry((dest & (rows * ny * nz - 1)) + 1, hot1[...])
    hxr[0] = head[:, 0:cx]
    for k in range(1, nx):
        hxs[k] = head[:, k * cx : (k + 1) * cx]
    fetches[1].wait()
    spread_rewards(hot1[...], rw_ref[...], nx, rxr.at[0], rxs.at[0])
    spread_rewards(hot1[...], swap(rw_ref[...]), nx, rxr.at[1], rxs.at[1])
    def send_rewards(axis, hop, half, out, into):
        for k in far_first(ring[axis][1]):
            at = 2 * hop + half
            send(axis, k, out.at[half, k], into.at[half, k], rsend.at[hop], rrecv.at[at])

    def drain_rewards(hop, half, ref):
        drain(ref.at[half, pl.ds(1, ref.shape[1] - 1)], rrecv.at[2 * hop + half])

    pl.semaphore_wait(barrier, (nx - 1) + (ny - 1) + (nz - 1))
    for k in far_first(nx):
        send("gx", k, hxs.at[k], hxr.at[k], hsend.at[0], hrecv.at[0])
    send_rewards("gx", 0, 0, rxs, rxr)
    send_rewards("gx", 0, 1, rxs, rxr)
    fetches[2].wait()
    len_row = jnp.concatenate([len_ref[t : t + 1, :] for t in range(rows // LANES)], axis=1)
    lens[...] = jnp.broadcast_to(to_column(len_row.astype(F32)), (rows, LANES)).astype(jnp.int32)
    fetches[3].wait()
    fetches[4].wait()

    def to_x(c):
        columns = pl.ds(pl.multiple_of(c * LANES, LANES), LANES)
        inside = (iota((rows, LANES), 1) + c * LANES) < lens[...]
        policy = lp_ref[:, columns]
        gap = rp_ref[:, columns] - policy
        penalty = jnp.exp(gap) - gap - 1.0
        policy = jnp.where(inside, policy, 0.0)
        penalty = jnp.where(inside, BETA * penalty, 0.0)
        other = swap(policy)
        both = jnp.concatenate(
            [jnp.where(low(), penalty, other), jnp.where(low(), other, penalty)], axis=1
        )
        got = pick(hot1[...], both)
        for h in range(2):
            part = got[:, h * LANES : (h + 1) * LANES]
            xr[2 * c + h, 0:cx, :] = part[0:cx, :]
            xs[2 * c + h] = part
            for k in far_first(nx):
                at = pl.ds(k * cx, cx)
                send(
                    "gx", k, xs.at[2 * c + h, at], xr.at[2 * c + h, at],
                    xsend, xrecv.at[2 * c + h],
                )

    def to_y(c):
        drain(xr.at[c, pl.ds(cx, slots - cx)], xrecv.at[c])
        got = pick(hot2[...], xr[c])
        yr[c, 0:cy, :] = got[0:cy, :]
        ys[c] = got
        for k in far_first(ny):
            at = pl.ds(k * cy, cy)
            send("gy", k, ys.at[c, at], yr.at[c, at], ysend, yrecv.at[c])

    def drain_y(c):
        drain(yr.at[c, pl.ds(cy, slots - cy)], yrecv.at[c])

    def gather_z(c):
        drain_y(2 * c)
        drain_y(2 * c + 1)
        return pick(hot3[...], jnp.concatenate([yr[2 * c], yr[2 * c + 1]], axis=1))

    def loss(even, odd, weights):
        return jnp.where(low(), even, odd) - weights * swap(jnp.where(low(), odd, even))

    def send_z(c, rows_out):
        zr[c, 0:cz, :] = rows_out[0:cz, :]
        zs[c] = rows_out
        for k in far_first(nz):
            at = pl.ds(k * cz, cz)
            send("gz", k, zs.at[c, at], zr.at[c, at], zsend, zrecv.at[c])

    to_x(0)

    drain(hxr.at[pl.ds(1, nx - 1)], hrecv.at[0])
    head = jnp.concatenate([hxr[k] for k in range(nx)], axis=1)
    held = head.astype(jnp.int32)
    hot2[...] = one_hot(slots_of((held - 1) >> log2(rows * nz), held > 0, my, ny, cy), slots)
    head = carry(held, hot2[...])
    hyr[0] = head[:, 0:cy]
    for k in range(1, ny):
        hys[k] = head[:, k * cy : (k + 1) * cy]
    for k in far_first(ny):
        send("gy", k, hys.at[k], hyr.at[k], hsend.at[1], hrecv.at[1])

    for half in range(2):
        drain_rewards(0, half, rxr)
        spread_rewards(hot2[...], unpacked(rxr.at[half]), ny, ryr.at[half], rys.at[half])
        send_rewards("gy", 1, half, rys, ryr)

    to_x(1)

    drain(hyr.at[pl.ds(1, ny - 1)], hrecv.at[1])
    head = jnp.concatenate([hyr[k] for k in range(ny)], axis=1)
    held = head.astype(jnp.int32)
    hot3[...] = one_hot(
        slots_of(((held - 1) >> log2(rows)) & (nz - 1), held > 0, mz, nz, cz), slots
    )
    head = carry(held, hot3[...])
    hzr[0] = head[:, 0:LANES]
    for t in range(tiles):
        hzs[t] = head[:, t * LANES : (t + 1) * LANES]
    for k in far_first(nz):
        send("gz", k, hzs.at[k // per_tile], hzr.at[k], hsend.at[2], hrecv.at[2])

    def rewards_to_z(half):
        drain_rewards(1, half, ryr)
        spread_rewards(hot3[...], unpacked(ryr.at[half]), nz, rzr.at[half], rzs.at[half])
        send_rewards("gz", 2, half, rzs, rzr)

    rewards_to_z(0)
    to_y(0)
    rewards_to_z(1)
    to_x(2)
    to_y(1)
    to_x(3)
    fetches[5].wait()

    drain_y(0)
    send_z(0, pick(hot3[...], yr[0]))
    to_y(2)
    drain(hzr.at[pl.ds(1, nz - 1)], hrecv.at[2])
    held = along_slots(lambda k: hzr[k]).astype(jnp.int32)
    place = jnp.where(held > 0, (held - 1) & (rows - 1), -1)
    hot4[...] = jnp.where(iota((rows, slots), 0) == place, 1.0, 0.0).astype(BF16)
    to_y(3)

    drain_rewards(2, 0, rzr)
    judged = pick_half(hot4[...], unpacked(rzr.at[0]))
    drain_rewards(2, 1, rzr)
    judged = jnp.where(low(), judged, swap(pick_half(hot4[...], unpacked(rzr.at[1]))))
    grouped = judged.reshape(rows // GROUP, GROUP, LANES)
    centre = jnp.mean(grouped, axis=1, keepdims=True)
    deviation = grouped - centre
    spread = jnp.mean(deviation * deviation, axis=1, keepdims=True)
    advantages = (deviation / jnp.sqrt(spread + 1.0)).reshape(rows, LANES)
    weight = jnp.sum(advantages * mix_ref[...], axis=1, keepdims=True)
    row = jnp.sum(hot4[...].astype(F32) * weight, axis=0, keepdims=True)
    wr[0] = row[:, 0:LANES]
    for t in range(tiles):
        ws[t] = row[:, t * LANES : (t + 1) * LANES]
    for k in far_first(nz):
        send("gz", -k, ws.at[k // per_tile], wr.at[k], rsend.at[3], rrecv.at[6])
    drain_y(1)
    send_z(chunks, pick(hot3[...], yr[1]))
    adv_ref[...] = advantages
    to_x(4)
    wrow[...] = jnp.broadcast_to(weight, (rows, LANES))

    to_y(4)
    to_x(5)
    to_y(5)
    second = gather_z(1)
    to_y(6)
    drain(wr.at[pl.ds(1, nz - 1)], rrecv.at[6])
    wcol[...] = jnp.broadcast_to(to_column(along_slots(lambda k: wr[k])), (slots, LANES))
    send_z(1, loss(second[:, 0:LANES], second[:, LANES:], wcol[...]))
    to_x(6)
    to_y(7)
    to_x(7)

    def loss_to_z(c):
        got = gather_z(c)
        send_z(c, loss(got[:, 0:LANES], got[:, LANES:], wcol[...]))

    @pl.loop(2, chunks - 2)
    def _(c):
        loss_to_z(c)
        to_y(2 * c + 4)
        to_y(2 * c + 5)

    @pl.loop(chunks - 2, chunks)
    def _(c):
        loss_to_z(c)

    for i, (h, r, n) in enumerate(((hxr, rxr, nx), (hyr, ryr, ny), (hzr, rzr, nz))):
        drain(h.at[pl.ds(1, n - 1)], hsend.at[i])
        drain(r.at[:, pl.ds(1, n - 1)], rsend.at[i])
    drain(wr.at[pl.ds(1, nz - 1)], rsend.at[3])
    drain(xs.at[:, pl.ds(cx, slots - cx)], xsend)
    drain(ys.at[:, pl.ds(cy, slots - cy)], ysend)

    def arrived(c):
        drain(zr.at[c, pl.ds(cz, slots - cz)], zrecv.at[c])
        return pick(hot4[...], zr[c])

    even = arrived(0)
    tok_ref[:, 0:LANES] = loss(even, arrived(chunks), wrow[...])

    def finish(c):
        columns = pl.ds(pl.multiple_of(c * LANES, LANES), LANES)
        tok_ref[:, columns] = arrived(c)

    @pl.loop(1, chunks - 1)
    def _(c):
        finish(c)

    drain(zs.at[:, pl.ds(cz, slots - cz)], zsend)
    finish(chunks - 1)


def store(tok_ref, adv_ref, tok_hbm, adv_hbm, sems):
    copies = [
        pltpu.make_async_copy(tok_ref, tok_hbm, sems.at[0]),
        pltpu.make_async_copy(adv_ref, adv_hbm, sems.at[1]),
    ]
    for copy in copies:
        copy.start()
    for copy in copies:
        copy.wait()


def on_device(sizes, log_probs, ref_log_probs, rewards, destination, lengths, mixing):
    rows, width = log_probs.shape
    slots = 2 * rows
    chunks = width // LANES
    nx, ny, nz = sizes
    wide = pltpu.VMEM((2 * chunks, slots, LANES), F32)
    thin = pltpu.VMEM((chunks + 1, slots, LANES), F32)
    sem = pltpu.SemaphoreType.DMA

    def head_buffer(n):
        return pltpu.VMEM((n, 1, LANES), F32)

    def reward_buffer(n):
        return pltpu.VMEM((2, n, slots // n // 2, LANES), F32)

    token_loss, advantages = pl.pallas_call(
        functools.partial(kernel, sizes, chunks),
        out_shape=(pltpu.VMEM((rows, width), F32), pltpu.VMEM((rows, LANES), F32)),
        in_specs=[pl.BlockSpec(memory_space=pl.ANY)] * 6,
        out_specs=(pl.BlockSpec(memory_space=pltpu.VMEM),) * 2,
        scratch_shapes=[
            pltpu.VMEM((rows // LANES, LANES), jnp.int32),
            pltpu.VMEM((rows // LANES, LANES), jnp.int32),
            pltpu.VMEM((1, LANES), F32),
            pltpu.VMEM((rows, width), F32),
            pltpu.VMEM((rows, width), F32),
            pltpu.VMEM((rows, LANES), F32),
            pltpu.VMEM((slots, slots), BF16),
            pltpu.VMEM((slots, rows), BF16),
            pltpu.VMEM((slots, slots), BF16),
            pltpu.VMEM((slots, slots), BF16),
            pltpu.VMEM((rows, slots), BF16),
            pltpu.VMEM((rows, LANES), jnp.int32),
            pltpu.VMEM((slots, LANES), F32),
            pltpu.VMEM((rows, LANES), F32),
            head_buffer(nx), head_buffer(nx),
            head_buffer(ny), head_buffer(ny),
            head_buffer(slots // LANES), head_buffer(nz),
            head_buffer(slots // LANES), head_buffer(nz),
            reward_buffer(nx), reward_buffer(nx),
            reward_buffer(ny), reward_buffer(ny),
            reward_buffer(nz), reward_buffer(nz),
            wide, wide, wide, wide, thin, thin,
            sem((6,)), sem((3,)), sem((3,)), sem((4,)), sem((7,)),
            sem, sem((2 * chunks,)), sem, sem((2 * chunks,)), sem, sem((chunks + 1,)),
        ],
        compiler_params=pltpu.CompilerParams(
            collective_id=0, has_side_effects=True, vmem_limit_bytes=60 << 20
        ),
        name="regroup",
    )(
        destination.reshape(rows // LANES, LANES),
        lengths.reshape(rows // LANES, LANES),
        mixing.reshape(1, LANES),
        log_probs,
        ref_log_probs,
        rewards,
    )
    return pl.pallas_call(
        store,
        out_shape=(
            jax.ShapeDtypeStruct((rows, width), F32),
            jax.ShapeDtypeStruct((rows, LANES), F32),
        ),
        in_specs=[pl.BlockSpec(memory_space=pltpu.VMEM)] * 2,
        out_specs=(pl.BlockSpec(memory_space=pl.ANY),) * 2,
        scratch_shapes=[sem((2,))],
        name="store",
    )(
        pltpu.with_memory_space_constraint(token_loss, pltpu.VMEM),
        pltpu.with_memory_space_constraint(advantages, pltpu.VMEM),
    )


def solution(mesh):
    sizes = tuple(mesh.shape[a] for a in ("gx", "gy", "gz"))
    rows = P(("gx", "gy", "gz"), None)
    flat = P(("gx", "gy", "gz"))
    return jax.shard_map(
        functools.partial(on_device, sizes),
        mesh=mesh,
        in_specs=(rows, rows, rows, flat, flat, P()),
        out_specs=(rows, rows),
        check_vma=False,
    )
```

```python
import functools

import jax
import jax.numpy as jnp
from jax import lax
from jax.experimental import pallas as pl
from jax.experimental.pallas import tpu as pltpu
from jax.sharding import PartitionSpec as P

GROUP = 16
BETA = 0.2
LANES = 128
HALF = LANES // 2
HEAD = 8
MESH = pl.DeviceIdType.MESH
F32 = jnp.float32
BF16 = jnp.bfloat16


def log2(n):
    return n.bit_length() - 1


def iota(shape, dim):
    return lax.broadcasted_iota(jnp.int32, shape, dim)


def dot(a, b):
    return jnp.dot(a, b, preferred_element_type=F32)


def pick(onehot, x):
    n = x.shape[1]
    first = x.astype(BF16)
    second = (x - first.astype(F32)).astype(BF16)
    got = dot(onehot, jnp.concatenate([first, second], axis=1))
    return got[:, 0:n] + got[:, n:]


def low():
    return iota((1, LANES), 1) < HALF


def swap(x):
    return pltpu.roll(x, HALF, 1)


def pick_half(onehot, x):
    first = x.astype(BF16).astype(F32)
    rest = x - first
    second = rest.astype(BF16).astype(F32)
    third = (rest - second).astype(BF16)
    both = jnp.where(low(), first, swap(second)).astype(BF16)
    got = dot(onehot, jnp.concatenate([both, third], axis=1))
    return (got[:, 0:LANES] + swap(got[:, 0:LANES])) + got[:, LANES:]


def to_column(row):
    n = row.shape[1]
    parts = []
    for t in range(n // LANES):
        tile = row[:, t * LANES : (t + 1) * LANES]
        eye = iota((LANES, LANES), 0) == iota((LANES, LANES), 1)
        parts.append(
            jnp.sum(jnp.where(eye, jnp.broadcast_to(tile, (LANES, LANES)), 0.0), axis=1, keepdims=True)
        )
    return jnp.concatenate(parts, axis=0)


def kernel(
    sizes, chunks, dest_hbm, len_hbm, mix_hbm, lp_hbm, rp_hbm, rw_hbm, tok_ref, adv_ref,
    dest_ref, len_ref, mix_ref, lp_ref, rp_ref, rw_ref,
    upper, hot1, hot2, hot3, hot4, lens, wcol, wrow,
    hxs, hxr, hys, hyr, hzs, hzr, ws, wr,
    rxs, rxr, rys, ryr, rzs, rzr,
    xs, xr, ys, yr, zs, zr,
    loads, hsend, hrecv, rsend, rrecv, xsend, xrecv, ysend, yrecv, nsend, zsend, zrecv,
):
    nx, ny, nz = sizes
    rows = lp_ref.shape[0]
    slots = 2 * rows
    cx, cy, cz = slots // nx, slots // ny, slots // nz
    per_tile = LANES // cz
    tiles = slots // LANES
    mx, my, mz = lax.axis_index("gx"), lax.axis_index("gy"), lax.axis_index("gz")
    ring = {"gx": (mx, nx), "gy": (my, ny), "gz": (mz, nz)}

    def far_first(n):
        return sorted(range(1, n), key=lambda k: -min(k, n - k))

    near = [k for k in far_first(nz) if min(k, nz - k) <= 3]
    far = [k for k in far_first(nz) if k not in near]

    def peer(axis, step):
        me, n = ring[axis]
        return {axis: lax.rem(me + (step + n), n)}

    fetches = [
        pltpu.make_async_copy(a, b, loads.at[i])
        for i, (a, b) in enumerate(
            (
                (dest_hbm, dest_ref), (rw_hbm, rw_ref), (len_hbm, len_ref),
                (lp_hbm, lp_ref), (rp_hbm, rp_ref), (mix_hbm, mix_ref),
            )
        )
    ]
    barrier = pltpu.get_barrier_semaphore()
    for axis in ("gz", "gx", "gy"):
        for k in far_first(ring[axis][1]):
            pl.semaphore_signal(barrier, inc=1, device_id=peer(axis, k), device_id_type=MESH)

    for fetch in fetches:
        fetch.start()

    def send(axis, k, src, dst, ssem, rsem):
        pltpu.make_async_remote_copy(
            src_ref=src, dst_ref=dst, send_sem=ssem, recv_sem=rsem,
            device_id=peer(axis, k), device_id_type=MESH,
        ).start()

    def drain(ref, sem):
        pltpu.make_async_copy(ref, ref, sem).wait()

    upper[...] = jnp.where(iota((slots, slots), 0) < iota((slots, slots), 1), 1.0, 0.0).astype(BF16)

    def slots_of(digit, valid, me, fanout, capacity):
        n = digit.shape[1]
        step = lax.rem(digit - me + fanout, fanout)
        groups = max(fanout, 8)
        member = jnp.where((iota((groups, n), 0) == step) & valid, 1.0, 0.0)
        before = dot(member.astype(BF16), upper[0:n, 0:n])
        rank = jnp.sum(member * before, axis=0, keepdims=True).astype(jnp.int32)
        return jnp.where(valid, step * capacity + rank, -1)

    def one_hot(slot, count):
        n = slot.shape[1]
        return jnp.where(iota((count, n), 0) == slot, 1.0, 0.0).astype(BF16)

    def carry(head, hot):
        place = head - 1
        field = iota((HEAD, head.shape[1]), 0)
        parts = jnp.where(
            field == 0, place >> 8, jnp.where(field == 1, place & 255, jnp.where(field == 2, 1, 0))
        )
        parts = jnp.where(head > 0, parts, 0).astype(F32).astype(BF16)
        got = lax.dot_general(parts, hot, (((1,), (1,)), ((), ())), preferred_element_type=F32)
        return got[0:1, :] * 256.0 + got[1:2, :] + got[2:3, :]

    def spread_rewards(hot, x, n, own, out):
        got = pick_half(hot, x)
        c = slots // n // 2
        first = got.reshape(n, 2, c, LANES)[:, 0]
        last = swap(got).reshape(n, 2, c, LANES)[:, 1]
        packed = jnp.where(low()[None], first, last)
        own[0] = packed[0]
        out[...] = packed

    def unpacked(ref):
        n, c = ref.shape[0], ref.shape[1]
        x = ref[...]
        y = swap(x.reshape(n * c, LANES)).reshape(n, c, LANES)
        return jnp.concatenate([x, y], axis=1).reshape(slots, LANES)

    def along_slots(tile):
        spot = iota((1, LANES), 1) // cz
        parts = []
        for t in range(tiles):
            part = tile(t * per_tile)
            for j in range(1, per_tile):
                part = jnp.where(spot == j, tile(t * per_tile + j), part)
            parts.append(part)
        return jnp.concatenate(parts, axis=1)

    fetches[0].wait()
    dest = jnp.concatenate([dest_ref[t : t + 1, :] for t in range(rows // LANES)], axis=1)
    tx = dest >> log2(rows * ny * nz)
    hot1[...] = one_hot(slots_of(tx, dest >= 0, mx, nx, cx), slots)
    head = carry((dest & (rows * ny * nz - 1)) + 1, hot1[...])
    hxr[0] = head[:, 0:cx]
    for k in range(1, nx):
        hxs[k] = head[:, k * cx : (k + 1) * cx]
    fetches[1].wait()
    spread_rewards(hot1[...], rw_ref[...], nx, rxr.at[0], rxs.at[0])
    spread_rewards(hot1[...], swap(rw_ref[...]), nx, rxr.at[1], rxs.at[1])
    def send_rewards(axis, hop, half, out, into):
        for k in far_first(ring[axis][1]):
            at = 2 * hop + half
            send(axis, k, out.at[half, k], into.at[half, k], rsend.at[hop], rrecv.at[at])

    def drain_rewards(hop, half, ref):
        drain(ref.at[half, pl.ds(1, ref.shape[1] - 1)], rrecv.at[2 * hop + half])

    pl.semaphore_wait(barrier, (nx - 1) + (ny - 1) + (nz - 1))
    for k in far_first(nx):
        send("gx", k, hxs.at[k], hxr.at[k], hsend.at[0], hrecv.at[0])
    send_rewards("gx", 0, 0, rxs, rxr)
    send_rewards("gx", 0, 1, rxs, rxr)
    fetches[2].wait()
    len_row = jnp.concatenate([len_ref[t : t + 1, :] for t in range(rows // LANES)], axis=1)
    lens[...] = jnp.broadcast_to(to_column(len_row.astype(F32)), (rows, LANES)).astype(jnp.int32)
    fetches[3].wait()
    fetches[4].wait()

    def to_x(c):
        columns = pl.ds(pl.multiple_of(c * LANES, LANES), LANES)
        inside = (iota((rows, LANES), 1) + c * LANES) < lens[...]
        policy = lp_ref[:, columns]
        gap = rp_ref[:, columns] - policy
        penalty = jnp.exp(gap) - gap - 1.0
        policy = jnp.where(inside, policy, 0.0)
        penalty = jnp.where(inside, BETA * penalty, 0.0)
        other = swap(policy)
        both = jnp.concatenate(
            [jnp.where(low(), penalty, other), jnp.where(low(), other, penalty)], axis=1
        )
        got = pick(hot1[...], both)
        for h in range(2):
            part = got[:, h * LANES : (h + 1) * LANES]
            xr[2 * c + h, 0:cx, :] = part[0:cx, :]
            xs[2 * c + h] = part
            for k in far_first(nx):
                at = pl.ds(k * cx, cx)
                send(
                    "gx", k, xs.at[2 * c + h, at], xr.at[2 * c + h, at],
                    xsend, xrecv.at[2 * c + h],
                )

    def to_y(c):
        drain(xr.at[c, pl.ds(cx, slots - cx)], xrecv.at[c])
        got = pick(hot2[...], xr[c])
        yr[c, 0:cy, :] = got[0:cy, :]
        ys[c] = got
        for k in far_first(ny):
            at = pl.ds(k * cy, cy)
            send("gy", k, ys.at[c, at], yr.at[c, at], ysend, yrecv.at[c])

    def drain_y(c):
        drain(yr.at[c, pl.ds(cy, slots - cy)], yrecv.at[c])

    def gather_z(c):
        drain_y(2 * c)
        drain_y(2 * c + 1)
        return pick(hot3[...], jnp.concatenate([yr[2 * c], yr[2 * c + 1]], axis=1))

    def send_some(c, peers, sem_at):
        for k in peers:
            at = pl.ds(k * cz, cz)
            send("gz", k, zs.at[c, at], zr.at[c, at], nsend.at[sem_at], zrecv.at[c])

    def loss(even, odd, weights):
        return jnp.where(low(), even, odd) - weights * swap(jnp.where(low(), odd, even))

    def send_z(c, rows_out):
        zr[c, 0:cz, :] = rows_out[0:cz, :]
        zs[c] = rows_out
        for k in far_first(nz):
            at = pl.ds(k * cz, cz)
            send("gz", k, zs.at[c, at], zr.at[c, at], zsend, zrecv.at[c])

    to_x(0)

    drain(hxr.at[pl.ds(1, nx - 1)], hrecv.at[0])
    head = jnp.concatenate([hxr[k] for k in range(nx)], axis=1)
    held = head.astype(jnp.int32)
    hot2[...] = one_hot(slots_of((held - 1) >> log2(rows * nz), held > 0, my, ny, cy), slots)
    head = carry(held, hot2[...])
    hyr[0] = head[:, 0:cy]
    for k in range(1, ny):
        hys[k] = head[:, k * cy : (k + 1) * cy]
    for k in far_first(ny):
        send("gy", k, hys.at[k], hyr.at[k], hsend.at[1], hrecv.at[1])

    for half in range(2):
        drain_rewards(0, half, rxr)
        spread_rewards(hot2[...], unpacked(rxr.at[half]), ny, ryr.at[half], rys.at[half])
        send_rewards("gy", 1, half, rys, ryr)

    drain(hyr.at[pl.ds(1, ny - 1)], hrecv.at[1])
    head = jnp.concatenate([hyr[k] for k in range(ny)], axis=1)
    held = head.astype(jnp.int32)
    hot3[...] = one_hot(
        slots_of(((held - 1) >> log2(rows)) & (nz - 1), held > 0, mz, nz, cz), slots
    )
    head = carry(held, hot3[...])
    hzr[0] = head[:, 0:LANES]
    for t in range(tiles):
        hzs[t] = head[:, t * LANES : (t + 1) * LANES]
    for k in far_first(nz):
        send("gz", k, hzs.at[k // per_tile], hzr.at[k], hsend.at[2], hrecv.at[2])

    to_x(1)

    def rewards_to_z(half):
        drain_rewards(1, half, ryr)
        spread_rewards(hot3[...], unpacked(ryr.at[half]), nz, rzr.at[half], rzs.at[half])
        send_rewards("gz", 2, half, rzs, rzr)

    rewards_to_z(0)
    to_y(0)
    rewards_to_z(1)
    to_x(2)
    to_y(1)
    to_x(3)
    fetches[5].wait()

    drain_y(0)
    zs[0] = pick(hot3[...], yr[0])
    send_some(0, far, 0)
    to_y(2)
    drain(hzr.at[pl.ds(1, nz - 1)], hrecv.at[2])
    held = along_slots(lambda k: hzr[k]).astype(jnp.int32)
    place = jnp.where(held > 0, (held - 1) & (rows - 1), -1)
    hot4[...] = jnp.where(iota((rows, slots), 0) == place, 1.0, 0.0).astype(BF16)
    to_y(3)

    drain_rewards(2, 0, rzr)
    judged = pick_half(hot4[...], unpacked(rzr.at[0]))
    drain_rewards(2, 1, rzr)
    judged = jnp.where(low(), judged, swap(pick_half(hot4[...], unpacked(rzr.at[1]))))
    grouped = judged.reshape(rows // GROUP, GROUP, LANES)
    centre = jnp.mean(grouped, axis=1, keepdims=True)
    deviation = grouped - centre
    spread = jnp.mean(deviation * deviation, axis=1, keepdims=True)
    advantages = (deviation / jnp.sqrt(spread + 1.0)).reshape(rows, LANES)
    weight = jnp.sum(advantages * mix_ref[...], axis=1, keepdims=True)
    row = jnp.sum(hot4[...].astype(F32) * weight, axis=0, keepdims=True)
    wr[0] = row[:, 0:LANES]
    for t in range(tiles):
        ws[t] = row[:, t * LANES : (t + 1) * LANES]
    for k in far_first(nz):
        came = rrecv.at[6] if k in near else rrecv.at[7]
        send("gz", -k, ws.at[k // per_tile], wr.at[k], rsend.at[3], came)

    drain_y(1)
    zs[chunks] = pick(hot3[...], yr[1])
    send_some(chunks, far, 1)
    adv_ref[...] = advantages
    wrow[...] = jnp.broadcast_to(weight, (rows, LANES))
    to_x(4)
    to_y(4)
    to_x(5)

    drain(wr.at[pl.ds(0, len(near))], rrecv.at[6])
    none = jnp.zeros((1, LANES), F32)
    weights = to_column(along_slots(lambda k: none if k in far else wr[k]))
    first = loss(zs[0], zs[chunks], weights)
    zr[chunks + 1, 0:cz, :] = first[0:cz, :]
    zs[chunks + 1] = first
    send_some(chunks + 1, near, 2)
    to_y(5)
    second = gather_z(1)
    drain(wr.at[pl.ds(0, len(far))], rrecv.at[7])
    wcol[...] = jnp.broadcast_to(to_column(along_slots(lambda k: wr[k])), (slots, LANES))
    send_z(1, loss(second[:, 0:LANES], second[:, LANES:], wcol[...]))
    to_y(6)
    to_x(6)
    to_y(7)
    to_x(7)

    low_far, high_far = min(far) * cz, (max(far) + 1) * cz
    for c in (0, chunks):
        zr[c, 0:low_far, :] = jnp.zeros((low_far, LANES), F32)
        zr[c, high_far:slots, :] = jnp.zeros((slots - high_far, LANES), F32)
    zr[chunks + 1, low_far:high_far, :] = jnp.zeros((high_far - low_far, LANES), F32)

    def loss_to_z(c):
        got = gather_z(c)
        send_z(c, loss(got[:, 0:LANES], got[:, LANES:], wcol[...]))

    @pl.loop(2, chunks - 2)
    def _(c):
        loss_to_z(c)
        to_y(2 * c + 4)
        to_y(2 * c + 5)

    @pl.loop(chunks - 2, chunks)
    def _(c):
        loss_to_z(c)

    for i, (h, r, n) in enumerate(((hxr, rxr, nx), (hyr, ryr, ny), (hzr, rzr, nz))):
        drain(h.at[pl.ds(1, n - 1)], hsend.at[i])
        drain(r.at[:, pl.ds(1, n - 1)], rsend.at[i])
    drain(wr.at[pl.ds(1, nz - 1)], rsend.at[3])
    drain(xs.at[:, pl.ds(cx, slots - cx)], xsend)
    drain(ys.at[:, pl.ds(cy, slots - cy)], ysend)

    for c, peers in ((0, far), (chunks, far), (chunks + 1, near)):
        drain(zr.at[c, pl.ds(0, len(peers) * cz)], zrecv.at[c])
    first = loss(pick(hot4[...], zr[0]), pick(hot4[...], zr[chunks]), wrow[...])
    tok_ref[:, 0:LANES] = first + pick(hot4[...], zr[chunks + 1])

    def arrived(c):
        drain(zr.at[c, pl.ds(cz, slots - cz)], zrecv.at[c])
        return pick(hot4[...], zr[c])

    def finish(c):
        columns = pl.ds(pl.multiple_of(c * LANES, LANES), LANES)
        tok_ref[:, columns] = arrived(c)

    @pl.loop(1, chunks - 1)
    def _(c):
        finish(c)

    for i, peers in enumerate((far, far, near)):
        drain(zs.at[0, pl.ds(0, len(peers) * cz)], nsend.at[i])
    drain(zs.at[pl.ds(1, chunks - 1), pl.ds(cz, slots - cz)], zsend)
    finish(chunks - 1)


def store(tok_ref, adv_ref, tok_hbm, adv_hbm, sems):
    copies = [
        pltpu.make_async_copy(tok_ref, tok_hbm, sems.at[0]),
        pltpu.make_async_copy(adv_ref, adv_hbm, sems.at[1]),
    ]
    for copy in copies:
        copy.start()
    for copy in copies:
        copy.wait()


def on_device(sizes, log_probs, ref_log_probs, rewards, destination, lengths, mixing):
    rows, width = log_probs.shape
    slots = 2 * rows
    chunks = width // LANES
    nx, ny, nz = sizes
    wide = pltpu.VMEM((2 * chunks, slots, LANES), F32)
    thin = pltpu.VMEM((chunks + 2, slots, LANES), F32)
    sem = pltpu.SemaphoreType.DMA

    def head_buffer(n):
        return pltpu.VMEM((n, 1, LANES), F32)

    def reward_buffer(n):
        return pltpu.VMEM((2, n, slots // n // 2, LANES), F32)

    token_loss, advantages = pl.pallas_call(
        functools.partial(kernel, sizes, chunks),
        out_shape=(pltpu.VMEM((rows, width), F32), pltpu.VMEM((rows, LANES), F32)),
        in_specs=[pl.BlockSpec(memory_space=pl.ANY)] * 6,
        out_specs=(pl.BlockSpec(memory_space=pltpu.VMEM),) * 2,
        scratch_shapes=[
            pltpu.VMEM((rows // LANES, LANES), jnp.int32),
            pltpu.VMEM((rows // LANES, LANES), jnp.int32),
            pltpu.VMEM((1, LANES), F32),
            pltpu.VMEM((rows, width), F32),
            pltpu.VMEM((rows, width), F32),
            pltpu.VMEM((rows, LANES), F32),
            pltpu.VMEM((slots, slots), BF16),
            pltpu.VMEM((slots, rows), BF16),
            pltpu.VMEM((slots, slots), BF16),
            pltpu.VMEM((slots, slots), BF16),
            pltpu.VMEM((rows, slots), BF16),
            pltpu.VMEM((rows, LANES), jnp.int32),
            pltpu.VMEM((slots, LANES), F32),
            pltpu.VMEM((rows, LANES), F32),
            head_buffer(nx), head_buffer(nx),
            head_buffer(ny), head_buffer(ny),
            head_buffer(slots // LANES), head_buffer(nz),
            head_buffer(slots // LANES), head_buffer(nz),
            reward_buffer(nx), reward_buffer(nx),
            reward_buffer(ny), reward_buffer(ny),
            reward_buffer(nz), reward_buffer(nz),
            wide, wide, wide, wide, thin, thin,
            sem((6,)), sem((3,)), sem((3,)), sem((4,)), sem((8,)),
            sem, sem((2 * chunks,)), sem, sem((2 * chunks,)), sem((3,)), sem, sem((chunks + 2,)),
        ],
        compiler_params=pltpu.CompilerParams(
            collective_id=0, has_side_effects=True, vmem_limit_bytes=60 << 20
        ),
        name="regroup",
    )(
        destination.reshape(rows // LANES, LANES),
        lengths.reshape(rows // LANES, LANES),
        mixing.reshape(1, LANES),
        log_probs,
        ref_log_probs,
        rewards,
    )
    return pl.pallas_call(
        store,
        out_shape=(
            jax.ShapeDtypeStruct((rows, width), F32),
            jax.ShapeDtypeStruct((rows, LANES), F32),
        ),
        in_specs=[pl.BlockSpec(memory_space=pltpu.VMEM)] * 2,
        out_specs=(pl.BlockSpec(memory_space=pl.ANY),) * 2,
        scratch_shapes=[sem((2,))],
        name="store",
    )(
        pltpu.with_memory_space_constraint(token_loss, pltpu.VMEM),
        pltpu.with_memory_space_constraint(advantages, pltpu.VMEM),
    )


def solution(mesh):
    sizes = tuple(mesh.shape[a] for a in ("gx", "gy", "gz"))
    rows = P(("gx", "gy", "gz"), None)
    flat = P(("gx", "gy", "gz"))
    return jax.shard_map(
        functools.partial(on_device, sizes),
        mesh=mesh,
        in_specs=(rows, rows, rows, flat, flat, P()),
        out_specs=(rows, rows),
        check_vma=False,
    )
```

```python
import functools

import jax
import jax.numpy as jnp
from jax import lax
from jax.experimental import pallas as pl
from jax.experimental.pallas import tpu as pltpu
from jax.sharding import PartitionSpec as P

GROUP = 16
BETA = 0.2
LANES = 128
HALF = LANES // 2
HEAD = 8
MESH = pl.DeviceIdType.MESH
F32 = jnp.float32
BF16 = jnp.bfloat16


def log2(n):
    return n.bit_length() - 1


def iota(shape, dim):
    return lax.broadcasted_iota(jnp.int32, shape, dim)


def dot(a, b):
    return jnp.dot(a, b, preferred_element_type=F32)


def pick(onehot, x):
    n = x.shape[1]
    first = x.astype(BF16)
    second = (x - first.astype(F32)).astype(BF16)
    got = dot(onehot, jnp.concatenate([first, second], axis=1))
    return got[:, 0:n] + got[:, n:]


def low():
    return iota((1, LANES), 1) < HALF


def swap(x):
    return pltpu.roll(x, HALF, 1)


def pick_half(onehot, x):
    first = x.astype(BF16).astype(F32)
    rest = x - first
    second = rest.astype(BF16).astype(F32)
    third = (rest - second).astype(BF16)
    both = jnp.where(low(), first, swap(second)).astype(BF16)
    got = dot(onehot, jnp.concatenate([both, third], axis=1))
    return (got[:, 0:LANES] + swap(got[:, 0:LANES])) + got[:, LANES:]


def to_column(row):
    n = row.shape[1]
    parts = []
    for t in range(n // LANES):
        tile = row[:, t * LANES : (t + 1) * LANES]
        eye = iota((LANES, LANES), 0) == iota((LANES, LANES), 1)
        parts.append(
            jnp.sum(jnp.where(eye, jnp.broadcast_to(tile, (LANES, LANES)), 0.0), axis=1, keepdims=True)
        )
    return jnp.concatenate(parts, axis=0)


def kernel(
    sizes, chunks, dest_hbm, len_hbm, mix_hbm, lp_hbm, rp_hbm, rw_hbm, tok_ref, adv_ref,
    dest_ref, len_ref, mix_ref, lp_ref, rp_ref, rw_ref,
    upper, hot1, hot2, hot3, hot4, lens, wcol, wrow,
    hxs, hxr, hys, hyr, hzs, hzr, ws, wr,
    rxs, rxr, rys, ryr, rzs, rzr,
    xs, xr, ys, yr, zs, zr,
    loads, hsend, hrecv, rsend, rrecv, xsend, xrecv, ysend, yrecv, nsend, zsend, zrecv,
):
    nx, ny, nz = sizes
    rows = lp_ref.shape[0]
    slots = 2 * rows
    cx, cy, cz = slots // nx, slots // ny, slots // nz
    per_tile = LANES // cz
    tiles = slots // LANES
    mx, my, mz = lax.axis_index("gx"), lax.axis_index("gy"), lax.axis_index("gz")
    ring = {"gx": (mx, nx), "gy": (my, ny), "gz": (mz, nz)}

    def far_first(n):
        return [1, 3, 2] if n == 4 else sorted(range(1, n), key=lambda k: -min(k, n - k))

    near = [k for k in far_first(nz) if min(k, nz - k) <= 3]
    far = [k for k in far_first(nz) if k not in near]

    def peer(axis, step):
        me, n = ring[axis]
        return {axis: lax.rem(me + (step + n), n)}

    fetches = [
        pltpu.make_async_copy(a, b, loads.at[i])
        for i, (a, b) in enumerate(
            (
                (dest_hbm, dest_ref), (rw_hbm, rw_ref), (len_hbm, len_ref),
                (lp_hbm, lp_ref), (rp_hbm, rp_ref), (mix_hbm, mix_ref),
            )
        )
    ]
    barrier = pltpu.get_barrier_semaphore()
    for axis in ("gz", "gx", "gy"):
        for k in far_first(ring[axis][1]):
            pl.semaphore_signal(barrier, inc=1, device_id=peer(axis, k), device_id_type=MESH)

    for fetch in fetches:
        fetch.start()

    def send(axis, k, src, dst, ssem, rsem):
        pltpu.make_async_remote_copy(
            src_ref=src, dst_ref=dst, send_sem=ssem, recv_sem=rsem,
            device_id=peer(axis, k), device_id_type=MESH,
        ).start()

    def drain(ref, sem):
        pltpu.make_async_copy(ref, ref, sem).wait()

    upper[...] = jnp.where(iota((slots, slots), 0) < iota((slots, slots), 1), 1.0, 0.0).astype(BF16)

    def slots_of(digit, valid, me, fanout, capacity):
        n = digit.shape[1]
        step = lax.rem(digit - me + fanout, fanout)
        groups = max(fanout, 8)
        member = jnp.where((iota((groups, n), 0) == step) & valid, 1.0, 0.0)
        before = dot(member.astype(BF16), upper[0:n, 0:n])
        rank = jnp.sum(member * before, axis=0, keepdims=True).astype(jnp.int32)
        return jnp.where(valid, step * capacity + rank, -1)

    def one_hot(slot, count):
        n = slot.shape[1]
        return jnp.where(iota((count, n), 0) == slot, 1.0, 0.0).astype(BF16)

    def carry(head, hot):
        place = head - 1
        field = iota((HEAD, head.shape[1]), 0)
        parts = jnp.where(
            field == 0, place >> 8, jnp.where(field == 1, place & 255, jnp.where(field == 2, 1, 0))
        )
        parts = jnp.where(head > 0, parts, 0).astype(F32).astype(BF16)
        got = lax.dot_general(parts, hot, (((1,), (1,)), ((), ())), preferred_element_type=F32)
        return got[0:1, :] * 256.0 + got[1:2, :] + got[2:3, :]

    def spread_rewards(hot, x, n, own, out):
        got = pick_half(hot, x)
        c = slots // n // 2
        first = got.reshape(n, 2, c, LANES)[:, 0]
        last = swap(got).reshape(n, 2, c, LANES)[:, 1]
        packed = jnp.where(low()[None], first, last)
        own[0] = packed[0]
        out[...] = packed

    def unpacked(ref):
        n, c = ref.shape[0], ref.shape[1]
        x = ref[...]
        y = swap(x.reshape(n * c, LANES)).reshape(n, c, LANES)
        return jnp.concatenate([x, y], axis=1).reshape(slots, LANES)

    def along_slots(tile):
        spot = iota((1, LANES), 1) // cz
        parts = []
        for t in range(tiles):
            part = tile(t * per_tile)
            for j in range(1, per_tile):
                part = jnp.where(spot == j, tile(t * per_tile + j), part)
            parts.append(part)
        return jnp.concatenate(parts, axis=1)

    fetches[0].wait()
    dest = jnp.concatenate([dest_ref[t : t + 1, :] for t in range(rows // LANES)], axis=1)
    tx = dest >> log2(rows * ny * nz)
    hot1[...] = one_hot(slots_of(tx, dest >= 0, mx, nx, cx), slots)
    head = carry((dest & (rows * ny * nz - 1)) + 1, hot1[...])
    hxr[0] = head[:, 0:cx]
    for k in range(1, nx):
        hxs[k] = head[:, k * cx : (k + 1) * cx]
    fetches[1].wait()
    spread_rewards(hot1[...], rw_ref[...], nx, rxr.at[0], rxs.at[0])
    spread_rewards(hot1[...], swap(rw_ref[...]), nx, rxr.at[1], rxs.at[1])
    def send_rewards(axis, hop, half, out, into):
        for k in far_first(ring[axis][1]):
            at = 2 * hop + half
            send(axis, k, out.at[half, k], into.at[half, k], rsend.at[hop], rrecv.at[at])

    def drain_rewards(hop, half, ref):
        drain(ref.at[half, pl.ds(1, ref.shape[1] - 1)], rrecv.at[2 * hop + half])

    pl.semaphore_wait(barrier, (nx - 1) + (ny - 1) + (nz - 1))
    for k in far_first(nx):
        send("gx", k, hxs.at[k], hxr.at[k], hsend.at[0], hrecv.at[0])
    send_rewards("gx", 0, 0, rxs, rxr)
    send_rewards("gx", 0, 1, rxs, rxr)
    fetches[2].wait()
    len_row = jnp.concatenate([len_ref[t : t + 1, :] for t in range(rows // LANES)], axis=1)
    lens[...] = jnp.broadcast_to(to_column(len_row.astype(F32)), (rows, LANES)).astype(jnp.int32)
    fetches[3].wait()
    fetches[4].wait()

    def to_x(c):
        columns = pl.ds(pl.multiple_of(c * LANES, LANES), LANES)
        inside = (iota((rows, LANES), 1) + c * LANES) < lens[...]
        policy = lp_ref[:, columns]
        gap = rp_ref[:, columns] - policy
        penalty = jnp.exp(gap) - gap - 1.0
        policy = jnp.where(inside, policy, 0.0)
        penalty = jnp.where(inside, BETA * penalty, 0.0)
        other = swap(policy)
        both = jnp.concatenate(
            [jnp.where(low(), penalty, other), jnp.where(low(), other, penalty)], axis=1
        )
        got = pick(hot1[...], both)
        for h in range(2):
            part = got[:, h * LANES : (h + 1) * LANES]
            xr[2 * c + h, 0:cx, :] = part[0:cx, :]
            xs[2 * c + h] = part
            for k in far_first(nx):
                at = pl.ds(k * cx, cx)
                send(
                    "gx", k, xs.at[2 * c + h, at], xr.at[2 * c + h, at],
                    xsend, xrecv.at[2 * c + h],
                )

    def to_y(c, pair):
        drain(xr.at[c, pl.ds(cx, slots - cx)], xrecv.at[c])
        got = pick(hot2[...], xr[c])
        yr[c, 0:cy, :] = got[0:cy, :]
        ys[c] = got
        for k in far_first(ny):
            at = pl.ds(k * cy, cy)
            send("gy", k, ys.at[c, at], yr.at[c, at], ysend, yrecv.at[pair])

    def gather_z(c):
        drain(yr.at[pl.ds(2 * c, 2), pl.ds(cy, slots - cy)], yrecv.at[c])
        return pick(hot3[...], jnp.concatenate([yr[2 * c], yr[2 * c + 1]], axis=1))

    def send_some(c, peers, sem_at):
        for k in peers:
            at = pl.ds(k * cz, cz)
            send("gz", k, zs.at[c, at], zr.at[c, at], nsend.at[sem_at], zrecv.at[c])

    def loss(even, odd, weights):
        return jnp.where(low(), even, odd) - weights * swap(jnp.where(low(), odd, even))

    def send_z(c, rows_out):
        zr[c, 0:cz, :] = rows_out[0:cz, :]
        zs[c] = rows_out
        for k in far_first(nz):
            at = pl.ds(k * cz, cz)
            send("gz", k, zs.at[c, at], zr.at[c, at], zsend, zrecv.at[c])

    to_x(0)

    drain(hxr.at[pl.ds(1, nx - 1)], hrecv.at[0])
    head = jnp.concatenate([hxr[k] for k in range(nx)], axis=1)
    held = head.astype(jnp.int32)
    hot2[...] = one_hot(slots_of((held - 1) >> log2(rows * nz), held > 0, my, ny, cy), slots)
    head = carry(held, hot2[...])
    hyr[0] = head[:, 0:cy]
    for k in range(1, ny):
        hys[k] = head[:, k * cy : (k + 1) * cy]
    for k in far_first(ny):
        send("gy", k, hys.at[k], hyr.at[k], hsend.at[1], hrecv.at[1])

    for half in range(2):
        drain_rewards(0, half, rxr)
        spread_rewards(hot2[...], unpacked(rxr.at[half]), ny, ryr.at[half], rys.at[half])
        send_rewards("gy", 1, half, rys, ryr)

    drain(hyr.at[pl.ds(1, ny - 1)], hrecv.at[1])
    head = jnp.concatenate([hyr[k] for k in range(ny)], axis=1)
    held = head.astype(jnp.int32)
    hot3[...] = one_hot(
        slots_of(((held - 1) >> log2(rows)) & (nz - 1), held > 0, mz, nz, cz), slots
    )
    head = carry(held, hot3[...])
    hzr[0] = head[:, 0:LANES]
    for t in range(tiles):
        hzs[t] = head[:, t * LANES : (t + 1) * LANES]
    for k in far_first(nz):
        send("gz", k, hzs.at[k // per_tile], hzr.at[k], hsend.at[2], hrecv.at[2])

    to_x(1)

    def rewards_to_z(half):
        drain_rewards(1, half, ryr)
        spread_rewards(hot3[...], unpacked(ryr.at[half]), nz, rzr.at[half], rzs.at[half])
        send_rewards("gz", 2, half, rzs, rzr)

    rewards_to_z(0)
    to_y(0, 0)
    rewards_to_z(1)
    to_x(2)
    to_y(1, chunks)
    to_x(3)
    fetches[5].wait()

    drain(yr.at[0, pl.ds(cy, slots - cy)], yrecv.at[0])
    zs[0] = pick(hot3[...], yr[0])
    send_some(0, far, 0)
    to_y(2, 1)
    drain(hzr.at[pl.ds(1, nz - 1)], hrecv.at[2])
    held = along_slots(lambda k: hzr[k]).astype(jnp.int32)
    place = jnp.where(held > 0, (held - 1) & (rows - 1), -1)
    hot4[...] = jnp.where(iota((rows, slots), 0) == place, 1.0, 0.0).astype(BF16)
    to_y(3, 1)

    drain_rewards(2, 0, rzr)
    judged = pick_half(hot4[...], unpacked(rzr.at[0]))
    drain_rewards(2, 1, rzr)
    judged = jnp.where(low(), judged, swap(pick_half(hot4[...], unpacked(rzr.at[1]))))
    grouped = judged.reshape(rows // GROUP, GROUP, LANES)
    centre = jnp.mean(grouped, axis=1, keepdims=True)
    deviation = grouped - centre
    spread = jnp.mean(deviation * deviation, axis=1, keepdims=True)
    advantages = (deviation / jnp.sqrt(spread + 1.0)).reshape(rows, LANES)
    weight = jnp.sum(advantages * mix_ref[...], axis=1, keepdims=True)
    row = jnp.sum(hot4[...].astype(F32) * weight, axis=0, keepdims=True)
    wr[0] = row[:, 0:LANES]
    for t in range(tiles):
        ws[t] = row[:, t * LANES : (t + 1) * LANES]
    for k in far_first(nz):
        came = rrecv.at[6] if k in near else rrecv.at[7]
        send("gz", -k, ws.at[k // per_tile], wr.at[k], rsend.at[3], came)

    drain(yr.at[1, pl.ds(cy, slots - cy)], yrecv.at[chunks])
    zs[chunks] = pick(hot3[...], yr[1])
    send_some(chunks, far, 1)
    adv_ref[...] = advantages
    wrow[...] = jnp.broadcast_to(weight, (rows, LANES))
    to_x(4)
    to_y(4, 2)
    to_x(5)

    drain(wr.at[pl.ds(0, len(near))], rrecv.at[6])
    none = jnp.zeros((1, LANES), F32)
    weights = to_column(along_slots(lambda k: none if k in far else wr[k]))
    first = loss(zs[0], zs[chunks], weights)
    zr[chunks + 1, 0:cz, :] = first[0:cz, :]
    zs[chunks + 1] = first
    send_some(chunks + 1, near, 2)
    to_y(5, 2)
    second = gather_z(1)
    drain(wr.at[pl.ds(0, len(far))], rrecv.at[7])
    wcol[...] = jnp.broadcast_to(to_column(along_slots(lambda k: wr[k])), (slots, LANES))
    send_z(1, loss(second[:, 0:LANES], second[:, LANES:], wcol[...]))
    to_y(6, 3)
    to_x(6)
    to_y(7, 3)
    to_x(7)

    low_far, high_far = min(far) * cz, (max(far) + 1) * cz
    for c in (0, chunks):
        zr[c, 0:low_far, :] = jnp.zeros((low_far, LANES), F32)
        zr[c, high_far:slots, :] = jnp.zeros((slots - high_far, LANES), F32)
    zr[chunks + 1, low_far:high_far, :] = jnp.zeros((high_far - low_far, LANES), F32)

    def loss_to_z(c):
        got = gather_z(c)
        send_z(c, loss(got[:, 0:LANES], got[:, LANES:], wcol[...]))

    @pl.loop(2, chunks - 2)
    def _(c):
        loss_to_z(c)
        to_y(2 * c + 4, c + 2)
        to_y(2 * c + 5, c + 2)

    @pl.loop(chunks - 2, chunks)
    def _(c):
        loss_to_z(c)

    for i, (h, r, n) in enumerate(((hxr, rxr, nx), (hyr, ryr, ny), (hzr, rzr, nz))):
        drain(h.at[pl.ds(1, n - 1)], hsend.at[i])
        drain(r.at[:, pl.ds(1, n - 1)], rsend.at[i])
    drain(wr.at[pl.ds(1, nz - 1)], rsend.at[3])
    drain(xs.at[:, pl.ds(cx, slots - cx)], xsend)
    drain(ys.at[:, pl.ds(cy, slots - cy)], ysend)

    for c, peers in ((0, far), (chunks, far), (chunks + 1, near)):
        drain(zr.at[c, pl.ds(0, len(peers) * cz)], zrecv.at[c])
    first = loss(pick(hot4[...], zr[0]), pick(hot4[...], zr[chunks]), wrow[...])
    tok_ref[:, 0:LANES] = first + pick(hot4[...], zr[chunks + 1])

    def arrived(c):
        drain(zr.at[c, pl.ds(cz, slots - cz)], zrecv.at[c])
        return pick(hot4[...], zr[c])

    def finish(c):
        columns = pl.ds(pl.multiple_of(c * LANES, LANES), LANES)
        tok_ref[:, columns] = arrived(c)

    @pl.loop(1, chunks - 1)
    def _(c):
        finish(c)

    for i, peers in enumerate((far, far, near)):
        drain(zs.at[0, pl.ds(0, len(peers) * cz)], nsend.at[i])
    drain(zs.at[pl.ds(1, chunks - 1), pl.ds(cz, slots - cz)], zsend)
    finish(chunks - 1)


def store(tok_ref, adv_ref, tok_hbm, adv_hbm, sems):
    copies = [
        pltpu.make_async_copy(tok_ref, tok_hbm, sems.at[0]),
        pltpu.make_async_copy(adv_ref, adv_hbm, sems.at[1]),
    ]
    for copy in copies:
        copy.start()
    for copy in copies:
        copy.wait()


def on_device(sizes, log_probs, ref_log_probs, rewards, destination, lengths, mixing):
    rows, width = log_probs.shape
    slots = 2 * rows
    chunks = width // LANES
    nx, ny, nz = sizes
    wide = pltpu.VMEM((2 * chunks, slots, LANES), F32)
    thin = pltpu.VMEM((chunks + 2, slots, LANES), F32)
    sem = pltpu.SemaphoreType.DMA

    def head_buffer(n):
        return pltpu.VMEM((n, 1, LANES), F32)

    def reward_buffer(n):
        return pltpu.VMEM((2, n, slots // n // 2, LANES), F32)

    token_loss, advantages = pl.pallas_call(
        functools.partial(kernel, sizes, chunks),
        out_shape=(pltpu.VMEM((rows, width), F32), pltpu.VMEM((rows, LANES), F32)),
        in_specs=[pl.BlockSpec(memory_space=pl.ANY)] * 6,
        out_specs=(pl.BlockSpec(memory_space=pltpu.VMEM),) * 2,
        scratch_shapes=[
            pltpu.VMEM((rows // LANES, LANES), jnp.int32),
            pltpu.VMEM((rows // LANES, LANES), jnp.int32),
            pltpu.VMEM((1, LANES), F32),
            pltpu.VMEM((rows, width), F32),
            pltpu.VMEM((rows, width), F32),
            pltpu.VMEM((rows, LANES), F32),
            pltpu.VMEM((slots, slots), BF16),
            pltpu.VMEM((slots, rows), BF16),
            pltpu.VMEM((slots, slots), BF16),
            pltpu.VMEM((slots, slots), BF16),
            pltpu.VMEM((rows, slots), BF16),
            pltpu.VMEM((rows, LANES), jnp.int32),
            pltpu.VMEM((slots, LANES), F32),
            pltpu.VMEM((rows, LANES), F32),
            head_buffer(nx), head_buffer(nx),
            head_buffer(ny), head_buffer(ny),
            head_buffer(slots // LANES), head_buffer(nz),
            head_buffer(slots // LANES), head_buffer(nz),
            reward_buffer(nx), reward_buffer(nx),
            reward_buffer(ny), reward_buffer(ny),
            reward_buffer(nz), reward_buffer(nz),
            wide, wide, wide, wide, thin, thin,
            sem((6,)), sem((3,)), sem((3,)), sem((4,)), sem((8,)),
            sem, sem((2 * chunks,)), sem, sem((chunks + 1,)), sem((3,)), sem, sem((chunks + 2,)),
        ],
        compiler_params=pltpu.CompilerParams(
            collective_id=0, has_side_effects=True, vmem_limit_bytes=60 << 20
        ),
        name="regroup",
    )(
        destination.reshape(rows // LANES, LANES),
        lengths.reshape(rows // LANES, LANES),
        mixing.reshape(1, LANES),
        log_probs,
        ref_log_probs,
        rewards,
    )
    return pl.pallas_call(
        store,
        out_shape=(
            jax.ShapeDtypeStruct((rows, width), F32),
            jax.ShapeDtypeStruct((rows, LANES), F32),
        ),
        in_specs=[pl.BlockSpec(memory_space=pltpu.VMEM)] * 2,
        out_specs=(pl.BlockSpec(memory_space=pl.ANY),) * 2,
        scratch_shapes=[sem((2,))],
        name="store",
    )(
        pltpu.with_memory_space_constraint(token_loss, pltpu.VMEM),
        pltpu.with_memory_space_constraint(advantages, pltpu.VMEM),
    )


def solution(mesh):
    sizes = tuple(mesh.shape[a] for a in ("gx", "gy", "gz"))
    rows = P(("gx", "gy", "gz"), None)
    flat = P(("gx", "gy", "gz"))
    return jax.shard_map(
        functools.partial(on_device, sizes),
        mesh=mesh,
        in_specs=(rows, rows, rows, flat, flat, P()),
        out_specs=(rows, rows),
        check_vma=False,
    )
```

```python
import functools

import jax
import jax.numpy as jnp
from jax import lax
from jax.experimental import pallas as pl
from jax.experimental.pallas import tpu as pltpu
from jax.sharding import PartitionSpec as P

GROUP = 16
BETA = 0.2
LANES = 128
HALF = LANES // 2
HEAD = 8
MESH = pl.DeviceIdType.MESH
F32 = jnp.float32
BF16 = jnp.bfloat16


def log2(n):
    return n.bit_length() - 1


def iota(shape, dim):
    return lax.broadcasted_iota(jnp.int32, shape, dim)


def dot(a, b):
    return jnp.dot(a, b, preferred_element_type=F32)


def pick(onehot, x):
    n = x.shape[1]
    first = x.astype(BF16)
    second = (x - first.astype(F32)).astype(BF16)
    got = dot(onehot, jnp.concatenate([first, second], axis=1))
    return got[:, 0:n] + got[:, n:]


def low():
    return iota((1, LANES), 1) < HALF


def swap(x):
    return pltpu.roll(x, HALF, 1)


def pick_half(onehot, x):
    first = x.astype(BF16).astype(F32)
    got = dot(onehot, jnp.where(low(), first, swap(x - first)).astype(BF16))
    return got + swap(got)


def to_column(row):
    n = row.shape[1]
    parts = []
    for t in range(n // LANES):
        tile = row[:, t * LANES : (t + 1) * LANES]
        eye = iota((LANES, LANES), 0) == iota((LANES, LANES), 1)
        parts.append(
            jnp.sum(jnp.where(eye, jnp.broadcast_to(tile, (LANES, LANES)), 0.0), axis=1, keepdims=True)
        )
    return jnp.concatenate(parts, axis=0)


def kernel(
    sizes, chunks, dest_hbm, len_hbm, mix_hbm, lp_hbm, rp_hbm, rw_hbm, tok_ref, adv_ref,
    dest_ref, len_ref, mix_ref, lp_ref, rp_ref, rw_ref,
    upper, hot1, hot2, hot3, hot4, lens, wcol, wrow,
    hxs, hxr, hys, hyr, hzs, hzr, ws, wr,
    rxs, rxr, rys, ryr, rzs, rzr,
    xs, xr, ys, yr, zs, zr,
    loads, hsend, hrecv, rsend, rrecv, xsend, xrecv, ysend, yrecv, nsend, zsend, zrecv,
):
    nx, ny, nz = sizes
    rows = lp_ref.shape[0]
    slots = 2 * rows
    cx, cy, cz = slots // nx, slots // ny, slots // nz
    per_tile = LANES // cz
    tiles = slots // LANES
    mx, my, mz = lax.axis_index("gx"), lax.axis_index("gy"), lax.axis_index("gz")
    ring = {"gx": (mx, nx), "gy": (my, ny), "gz": (mz, nz)}

    def far_first(n):
        return [1, 3, 2] if n == 4 else sorted(range(1, n), key=lambda k: -min(k, n - k))

    near = [k for k in far_first(nz) if min(k, nz - k) <= 3]
    far = [k for k in far_first(nz) if k not in near]

    def peer(axis, step):
        me, n = ring[axis]
        return {axis: lax.rem(me + (step + n), n)}

    fetches = [
        pltpu.make_async_copy(a, b, loads.at[i])
        for i, (a, b) in enumerate(
            (
                (dest_hbm, dest_ref), (rw_hbm, rw_ref), (len_hbm, len_ref),
                (lp_hbm, lp_ref), (rp_hbm, rp_ref), (mix_hbm, mix_ref),
            )
        )
    ]
    barrier = pltpu.get_barrier_semaphore()
    for axis in ("gz", "gx", "gy"):
        for k in far_first(ring[axis][1]):
            pl.semaphore_signal(barrier, inc=1, device_id=peer(axis, k), device_id_type=MESH)

    for fetch in fetches:
        fetch.start()

    def send(axis, k, src, dst, ssem, rsem):
        pltpu.make_async_remote_copy(
            src_ref=src, dst_ref=dst, send_sem=ssem, recv_sem=rsem,
            device_id=peer(axis, k), device_id_type=MESH,
        ).start()

    def drain(ref, sem):
        pltpu.make_async_copy(ref, ref, sem).wait()

    upper[...] = jnp.where(iota((slots, slots), 0) < iota((slots, slots), 1), 1.0, 0.0).astype(BF16)

    def slots_of(digit, valid, me, fanout, capacity):
        n = digit.shape[1]
        step = lax.rem(digit - me + fanout, fanout)
        groups = max(fanout, 8)
        member = jnp.where((iota((groups, n), 0) == step) & valid, 1.0, 0.0)
        before = dot(member.astype(BF16), upper[0:n, 0:n])
        rank = jnp.sum(member * before, axis=0, keepdims=True).astype(jnp.int32)
        return jnp.where(valid, step * capacity + rank, -1)

    def one_hot(slot, count):
        n = slot.shape[1]
        return jnp.where(iota((count, n), 0) == slot, 1.0, 0.0).astype(BF16)

    def carry(head, hot):
        place = head - 1
        field = iota((HEAD, head.shape[1]), 0)
        parts = jnp.where(
            field == 0, place >> 8, jnp.where(field == 1, place & 255, jnp.where(field == 2, 1, 0))
        )
        parts = jnp.where(head > 0, parts, 0).astype(F32).astype(BF16)
        got = lax.dot_general(parts, hot, (((1,), (1,)), ((), ())), preferred_element_type=F32)
        return got[0:1, :] * 256.0 + got[1:2, :] + got[2:3, :]

    def spread_rewards(hot, x, n, own, out):
        got = pick_half(hot, x)
        c = slots // n // 2
        first = got.reshape(n, 2, c, LANES)[:, 0]
        last = swap(got).reshape(n, 2, c, LANES)[:, 1]
        packed = jnp.where(low()[None], first, last)
        own[0] = packed[0]
        out[...] = packed

    def unpacked(ref):
        n, c = ref.shape[0], ref.shape[1]
        x = ref[...]
        y = swap(x.reshape(n * c, LANES)).reshape(n, c, LANES)
        return jnp.concatenate([x, y], axis=1).reshape(slots, LANES)

    def along_slots(tile):
        spot = iota((1, LANES), 1) // cz
        parts = []
        for t in range(tiles):
            part = tile(t * per_tile)
            for j in range(1, per_tile):
                part = jnp.where(spot == j, tile(t * per_tile + j), part)
            parts.append(part)
        return jnp.concatenate(parts, axis=1)

    fetches[0].wait()
    dest = jnp.concatenate([dest_ref[t : t + 1, :] for t in range(rows // LANES)], axis=1)
    tx = dest >> log2(rows * ny * nz)
    hot1[...] = one_hot(slots_of(tx, dest >= 0, mx, nx, cx), slots)
    head = carry((dest & (rows * ny * nz - 1)) + 1, hot1[...])
    hxr[0] = head[:, 0:cx]
    for k in range(1, nx):
        hxs[k] = head[:, k * cx : (k + 1) * cx]
    fetches[1].wait()
    spread_rewards(hot1[...], rw_ref[...], nx, rxr.at[0], rxs.at[0])
    spread_rewards(hot1[...], swap(rw_ref[...]), nx, rxr.at[1], rxs.at[1])
    def send_rewards(axis, hop, half, out, into):
        for k in far_first(ring[axis][1]):
            at = 2 * hop + half
            send(axis, k, out.at[half, k], into.at[half, k], rsend.at[hop], rrecv.at[at])

    def drain_rewards(hop, half, ref):
        drain(ref.at[half, pl.ds(1, ref.shape[1] - 1)], rrecv.at[2 * hop + half])

    pl.semaphore_wait(barrier, (nx - 1) + (ny - 1) + (nz - 1))
    for k in far_first(nx):
        send("gx", k, hxs.at[k], hxr.at[k], hsend.at[0], hrecv.at[0])
    send_rewards("gx", 0, 0, rxs, rxr)
    send_rewards("gx", 0, 1, rxs, rxr)
    fetches[2].wait()
    len_row = jnp.concatenate([len_ref[t : t + 1, :] for t in range(rows // LANES)], axis=1)
    lens[...] = jnp.broadcast_to(to_column(len_row.astype(F32)), (rows, LANES)).astype(jnp.int32)
    fetches[3].wait()
    fetches[4].wait()

    def to_x(c):
        columns = pl.ds(pl.multiple_of(c * LANES, LANES), LANES)
        inside = (iota((rows, LANES), 1) + c * LANES) < lens[...]
        policy = lp_ref[:, columns]
        gap = rp_ref[:, columns] - policy
        penalty = jnp.exp(gap) - gap - 1.0
        policy = jnp.where(inside, policy, 0.0)
        penalty = jnp.where(inside, BETA * penalty, 0.0)
        other = swap(policy)
        both = jnp.concatenate(
            [jnp.where(low(), penalty, other), jnp.where(low(), other, penalty)], axis=1
        )
        got = pick(hot1[...], both)
        for h in range(2):
            part = got[:, h * LANES : (h + 1) * LANES]
            xr[2 * c + h, 0:cx, :] = part[0:cx, :]
            xs[2 * c + h] = part
            for k in far_first(nx):
                at = pl.ds(k * cx, cx)
                send(
                    "gx", k, xs.at[2 * c + h, at], xr.at[2 * c + h, at],
                    xsend, xrecv.at[2 * c + h],
                )

    def to_y(c, pair):
        drain(xr.at[c, pl.ds(cx, slots - cx)], xrecv.at[c])
        got = pick(hot2[...], xr[c])
        yr[c, 0:cy, :] = got[0:cy, :]
        ys[c] = got
        for k in far_first(ny):
            at = pl.ds(k * cy, cy)
            send("gy", k, ys.at[c, at], yr.at[c, at], ysend, yrecv.at[pair])

    def gather_z(c):
        drain(yr.at[pl.ds(2 * c, 2), pl.ds(cy, slots - cy)], yrecv.at[c])
        return pick(hot3[...], jnp.concatenate([yr[2 * c], yr[2 * c + 1]], axis=1))

    def send_some(c, peers, sem_at):
        for k in peers:
            at = pl.ds(k * cz, cz)
            send("gz", k, zs.at[c, at], zr.at[c, at], nsend.at[sem_at], zrecv.at[c])

    def loss(even, odd, weights):
        return jnp.where(low(), even, odd) - weights * swap(jnp.where(low(), odd, even))

    def send_z(c, rows_out):
        zr[c, 0:cz, :] = rows_out[0:cz, :]
        zs[c] = rows_out
        for k in far_first(nz):
            at = pl.ds(k * cz, cz)
            send("gz", k, zs.at[c, at], zr.at[c, at], zsend, zrecv.at[c])

    to_x(0)

    drain(hxr.at[pl.ds(1, nx - 1)], hrecv.at[0])
    head = jnp.concatenate([hxr[k] for k in range(nx)], axis=1)
    held = head.astype(jnp.int32)
    hot2[...] = one_hot(slots_of((held - 1) >> log2(rows * nz), held > 0, my, ny, cy), slots)
    head = carry(held, hot2[...])
    hyr[0] = head[:, 0:cy]
    for k in range(1, ny):
        hys[k] = head[:, k * cy : (k + 1) * cy]
    for k in far_first(ny):
        send("gy", k, hys.at[k], hyr.at[k], hsend.at[1], hrecv.at[1])

    for half in range(2):
        drain_rewards(0, half, rxr)
        spread_rewards(hot2[...], unpacked(rxr.at[half]), ny, ryr.at[half], rys.at[half])
        send_rewards("gy", 1, half, rys, ryr)

    drain(hyr.at[pl.ds(1, ny - 1)], hrecv.at[1])
    head = jnp.concatenate([hyr[k] for k in range(ny)], axis=1)
    held = head.astype(jnp.int32)
    hot3[...] = one_hot(
        slots_of(((held - 1) >> log2(rows)) & (nz - 1), held > 0, mz, nz, cz), slots
    )
    head = carry(held, hot3[...])
    hzr[0] = head[:, 0:LANES]
    for t in range(tiles):
        hzs[t] = head[:, t * LANES : (t + 1) * LANES]
    for k in far_first(nz):
        send("gz", k, hzs.at[k // per_tile], hzr.at[k], hsend.at[2], hrecv.at[2])

    to_x(1)

    def rewards_to_z(half):
        drain_rewards(1, half, ryr)
        spread_rewards(hot3[...], unpacked(ryr.at[half]), nz, rzr.at[half], rzs.at[half])
        send_rewards("gz", 2, half, rzs, rzr)

    rewards_to_z(0)
    to_y(0, 0)
    rewards_to_z(1)
    to_x(2)
    to_y(1, chunks)
    to_x(3)
    fetches[5].wait()

    drain(yr.at[0, pl.ds(cy, slots - cy)], yrecv.at[0])
    zs[0] = pick(hot3[...], yr[0])
    send_some(0, far, 0)
    to_y(2, 1)
    drain(hzr.at[pl.ds(1, nz - 1)], hrecv.at[2])
    held = along_slots(lambda k: hzr[k]).astype(jnp.int32)
    place = jnp.where(held > 0, (held - 1) & (rows - 1), -1)
    hot4[...] = jnp.where(iota((rows, slots), 0) == place, 1.0, 0.0).astype(BF16)
    to_y(3, 1)

    drain_rewards(2, 0, rzr)
    judged = pick_half(hot4[...], unpacked(rzr.at[0]))
    drain_rewards(2, 1, rzr)
    judged = jnp.where(low(), judged, swap(pick_half(hot4[...], unpacked(rzr.at[1]))))
    grouped = judged.reshape(rows // GROUP, GROUP, LANES)
    centre = jnp.mean(grouped, axis=1, keepdims=True)
    deviation = grouped - centre
    spread = jnp.mean(deviation * deviation, axis=1, keepdims=True)
    advantages = (deviation / jnp.sqrt(spread + 1.0)).reshape(rows, LANES)
    weight = jnp.sum(advantages * mix_ref[...], axis=1, keepdims=True)
    row = jnp.sum(hot4[...].astype(F32) * weight, axis=0, keepdims=True)
    wr[0] = row[:, 0:LANES]
    for t in range(tiles):
        ws[t] = row[:, t * LANES : (t + 1) * LANES]
    for k in far_first(nz):
        came = rrecv.at[6] if k in near else rrecv.at[7]
        send("gz", -k, ws.at[k // per_tile], wr.at[k], rsend.at[3], came)

    drain(yr.at[1, pl.ds(cy, slots - cy)], yrecv.at[chunks])
    zs[chunks] = pick(hot3[...], yr[1])
    send_some(chunks, far, 1)
    adv_ref[...] = advantages
    wrow[...] = jnp.broadcast_to(weight, (rows, LANES))
    to_x(4)
    to_y(4, 2)
    to_x(5)

    drain(wr.at[pl.ds(0, len(near))], rrecv.at[6])
    none = jnp.zeros((1, LANES), F32)
    weights = to_column(along_slots(lambda k: none if k in far else wr[k]))
    first = loss(zs[0], zs[chunks], weights)
    zr[chunks + 1, 0:cz, :] = first[0:cz, :]
    zs[chunks + 1] = first
    send_some(chunks + 1, near, 2)
    to_y(5, 2)
    second = gather_z(1)
    drain(wr.at[pl.ds(0, len(far))], rrecv.at[7])
    wcol[...] = jnp.broadcast_to(to_column(along_slots(lambda k: wr[k])), (slots, LANES))
    send_z(1, loss(second[:, 0:LANES], second[:, LANES:], wcol[...]))
    to_y(6, 3)
    to_x(6)
    to_y(7, 3)
    to_x(7)

    low_far, high_far = min(far) * cz, (max(far) + 1) * cz
    for c in (0, chunks):
        zr[c, 0:low_far, :] = jnp.zeros((low_far, LANES), F32)
        zr[c, high_far:slots, :] = jnp.zeros((slots - high_far, LANES), F32)
    zr[chunks + 1, low_far:high_far, :] = jnp.zeros((high_far - low_far, LANES), F32)

    def loss_to_z(c):
        got = gather_z(c)
        send_z(c, loss(got[:, 0:LANES], got[:, LANES:], wcol[...]))

    @pl.loop(2, chunks - 2)
    def _(c):
        loss_to_z(c)
        to_y(2 * c + 4, c + 2)
        to_y(2 * c + 5, c + 2)

    @pl.loop(chunks - 2, chunks)
    def _(c):
        loss_to_z(c)

    for i, (h, r, n) in enumerate(((hxr, rxr, nx), (hyr, ryr, ny), (hzr, rzr, nz))):
        drain(h.at[pl.ds(1, n - 1)], hsend.at[i])
        drain(r.at[:, pl.ds(1, n - 1)], rsend.at[i])
    drain(wr.at[pl.ds(1, nz - 1)], rsend.at[3])
    drain(xs.at[:, pl.ds(cx, slots - cx)], xsend)
    drain(ys.at[:, pl.ds(cy, slots - cy)], ysend)

    for c, peers in ((0, far), (chunks, far), (chunks + 1, near)):
        drain(zr.at[c, pl.ds(0, len(peers) * cz)], zrecv.at[c])
    first = loss(pick(hot4[...], zr[0]), pick(hot4[...], zr[chunks]), wrow[...])
    tok_ref[:, 0:LANES] = first + pick(hot4[...], zr[chunks + 1])

    def arrived(c):
        drain(zr.at[c, pl.ds(cz, slots - cz)], zrecv.at[c])
        return pick(hot4[...], zr[c])

    def finish(c):
        columns = pl.ds(pl.multiple_of(c * LANES, LANES), LANES)
        tok_ref[:, columns] = arrived(c)

    @pl.loop(1, chunks - 1)
    def _(c):
        finish(c)

    for i, peers in enumerate((far, far, near)):
        drain(zs.at[0, pl.ds(0, len(peers) * cz)], nsend.at[i])
    drain(zs.at[pl.ds(1, chunks - 1), pl.ds(cz, slots - cz)], zsend)
    finish(chunks - 1)


def store(tok_ref, adv_ref, tok_hbm, adv_hbm, sems):
    copies = [
        pltpu.make_async_copy(tok_ref, tok_hbm, sems.at[0]),
        pltpu.make_async_copy(adv_ref, adv_hbm, sems.at[1]),
    ]
    for copy in copies:
        copy.start()
    for copy in copies:
        copy.wait()


def on_device(sizes, log_probs, ref_log_probs, rewards, destination, lengths, mixing):
    rows, width = log_probs.shape
    slots = 2 * rows
    chunks = width // LANES
    nx, ny, nz = sizes
    wide = pltpu.VMEM((2 * chunks, slots, LANES), F32)
    thin = pltpu.VMEM((chunks + 2, slots, LANES), F32)
    sem = pltpu.SemaphoreType.DMA

    def head_buffer(n):
        return pltpu.VMEM((n, 1, LANES), F32)

    def reward_buffer(n):
        return pltpu.VMEM((2, n, slots // n // 2, LANES), F32)

    token_loss, advantages = pl.pallas_call(
        functools.partial(kernel, sizes, chunks),
        out_shape=(pltpu.VMEM((rows, width), F32), pltpu.VMEM((rows, LANES), F32)),
        in_specs=[pl.BlockSpec(memory_space=pl.ANY)] * 6,
        out_specs=(pl.BlockSpec(memory_space=pltpu.VMEM),) * 2,
        scratch_shapes=[
            pltpu.VMEM((rows // LANES, LANES), jnp.int32),
            pltpu.VMEM((rows // LANES, LANES), jnp.int32),
            pltpu.VMEM((1, LANES), F32),
            pltpu.VMEM((rows, width), F32),
            pltpu.VMEM((rows, width), F32),
            pltpu.VMEM((rows, LANES), F32),
            pltpu.VMEM((slots, slots), BF16),
            pltpu.VMEM((slots, rows), BF16),
            pltpu.VMEM((slots, slots), BF16),
            pltpu.VMEM((slots, slots), BF16),
            pltpu.VMEM((rows, slots), BF16),
            pltpu.VMEM((rows, LANES), jnp.int32),
            pltpu.VMEM((slots, LANES), F32),
            pltpu.VMEM((rows, LANES), F32),
            head_buffer(nx), head_buffer(nx),
            head_buffer(ny), head_buffer(ny),
            head_buffer(slots // LANES), head_buffer(nz),
            head_buffer(slots // LANES), head_buffer(nz),
            reward_buffer(nx), reward_buffer(nx),
            reward_buffer(ny), reward_buffer(ny),
            reward_buffer(nz), reward_buffer(nz),
            wide, wide, wide, wide, thin, thin,
            sem((6,)), sem((3,)), sem((3,)), sem((4,)), sem((8,)),
            sem, sem((2 * chunks,)), sem, sem((chunks + 1,)), sem((3,)), sem, sem((chunks + 2,)),
        ],
        compiler_params=pltpu.CompilerParams(
            collective_id=0, has_side_effects=True, vmem_limit_bytes=60 << 20
        ),
        name="regroup",
    )(
        destination.reshape(rows // LANES, LANES),
        lengths.reshape(rows // LANES, LANES),
        mixing.reshape(1, LANES),
        log_probs,
        ref_log_probs,
        rewards,
    )
    return pl.pallas_call(
        store,
        out_shape=(
            jax.ShapeDtypeStruct((rows, width), F32),
            jax.ShapeDtypeStruct((rows, LANES), F32),
        ),
        in_specs=[pl.BlockSpec(memory_space=pltpu.VMEM)] * 2,
        out_specs=(pl.BlockSpec(memory_space=pl.ANY),) * 2,
        scratch_shapes=[sem((2,))],
        name="store",
    )(
        pltpu.with_memory_space_constraint(token_loss, pltpu.VMEM),
        pltpu.with_memory_space_constraint(advantages, pltpu.VMEM),
    )


def solution(mesh):
    sizes = tuple(mesh.shape[a] for a in ("gx", "gy", "gz"))
    rows = P(("gx", "gy", "gz"), None)
    flat = P(("gx", "gy", "gz"))
    return jax.shard_map(
        functools.partial(on_device, sizes),
        mesh=mesh,
        in_specs=(rows, rows, rows, flat, flat, P()),
        out_specs=(rows, rows),
        check_vma=False,
    )
```
